32 devices in a mesh: seq: 8 (over z, y), head: 4 (over x, core).
Axes of the slice: x: 2, y: 2, z: 4, core: 2. Of those that a mesh axis runs over, the one named last changes fastest.
Arguments:
- query: bfloat16 [8, 40, 128], P(None, 'head'), may hold values from -400 to 400
- key_cache: bfloat16 [8, 4096, 8, 128], P(None, 'seq', 'head'), may hold values from -6 to 6
- value_cache: bfloat16 [8, 4096, 8, 128], P(None, 'seq', 'head'), may hold values from -6 to 6
- new_key: bfloat16 [8, 8, 128], P(None, 'head'), may hold values from -6 to 6
- new_value: bfloat16 [8, 8, 128], P(None, 'head'), may hold values from -6 to 6
- lengths: int32 [8], replicated, may hold values from 1024 to 4096, as said below
- out_weight: bfloat16 [5120, 5120], P('head', 'seq'), may hold values from -0.078125 to 0.078125
Outputs:
- projected: float32 [8, 5120], P(None, 'seq')
The draws below stay inside these ranges and needn't reach their ends.
Inputs may be any that keep to these rules, and one draw needn't show every extreme that they name: `lengths`: some sequence has exactly 4096 cached tokens.
All inputs are finite; a program needn't handle non-finite values.
Results may differ from the reference program's by a relative error of at most 0.0064.
Values sent between devices are 32-bit elements; how exact they have to be, the bound alone decides.
No kernel may reach another device: no remote copies, remote signals or barrier semaphores. Data moves between devices by JAX's collectives and lax.ppermute only.
A program may use at most 64 MiB of HBM per device.

```python
import math
import jax
import jax.numpy as jnp
from jax import lax

B = 8
HQ = 40
KVH = 8
HD = 128
D = 5120
POS_DEV = 512
CACHE = 4096
STRETCH = 512
GROUP = 5
N_SEQ = 8


def common_noise(key):
    return jax.random.normal(jax.random.fold_in(key, 7), (B, HQ, HD), jnp.float32)


def draw_query(key, part):
    base = common_noise(key)
    return jnp.clip(3.0 * base, -18.0, 18.0).astype(jnp.bfloat16)


def draw_new_key(key, part):
    base = common_noise(key)
    grouped = base.reshape(B, KVH, HQ // KVH, HD).mean(axis=2)
    noise = jax.random.normal(jax.random.fold_in(key, 8), (B, KVH, HD), jnp.float32)
    return jnp.clip(1.8 * grouped + 0.6 * noise, -6.0, 6.0).astype(jnp.bfloat16)


def draw_lengths(key, part):
    drawn = jax.random.randint(jax.random.fold_in(key, 11), (B,), CACHE // 4, CACHE)
    picked = jax.random.randint(jax.random.fold_in(key, 12), (), 0, B)
    return jnp.where(jnp.arange(B) == picked, CACHE, drawn).astype(jnp.int32)


def levels(own_key, dims, split, low, largest):
    def one(position, blocks):
        draws = jax.random.uniform(jax.random.fold_in(jax.random.fold_in(own_key, 6), position), (blocks,), jnp.float32, low / len(split), largest / len(split))
        return jnp.repeat(jnp.exp(draws), dims[position] // blocks).reshape((-1,) + (1,) * (len(dims) - position - 1))

    gain = one(*split[0])
    for cut in split[1:]:
        gain = gain * one(*cut)
    return gain


def normal_values(own_key, dims, deviation, bound, split=(), held_as=jnp.bfloat16):
    entries = deviation * jax.random.normal(own_key, dims, jnp.float32)
    if split:
        entries = entries * levels(own_key, dims, split, -0.22, 0.18)
    return jnp.clip(entries, -bound, bound).astype(held_as)


def setup_inputs(seed: int = 0) -> dict:
    arg_keys = jax.random.split(jax.random.key(seed), 8)
    query = draw_query(jax.random.fold_in(arg_keys[7], 71), 0)
    key_cache = normal_values(arg_keys[1], (B, CACHE, KVH, HD), 1.0, 6.0, ((1, 8), (2, 4)))
    value_cache = normal_values(arg_keys[2], (B, CACHE, KVH, HD), 1.0, 6.0, ((1, 8), (2, 4)))
    new_key = draw_new_key(jax.random.fold_in(arg_keys[7], 71), 0)
    new_value = normal_values(arg_keys[4], (B, KVH, HD), 1.0, 6.0, ((1, 4),))
    lengths = draw_lengths(jax.random.fold_in(arg_keys[7], 71), 0)
    out_weight = normal_values(arg_keys[6], (HQ * HD, D), (HQ * HD) ** -0.5, 0.078125, ((0, 4), (1, 8)))
    return dict(query=query, key_cache=key_cache, value_cache=value_cache, new_key=new_key, new_value=new_value, lengths=lengths, out_weight=out_weight)


THETA_BASE = 10000000.0
NEG_FILL = -1e+30

def apply_rotary(values, positions):
    half_width = values.shape[-1] // 2
    frequency = jnp.exp(jnp.arange(half_width, dtype=jnp.float32) * jnp.float32(-2.0 * math.log(THETA_BASE) / values.shape[-1]))
    angles = positions[..., None] * frequency
    cos_part = jnp.cos(angles)
    sin_part = jnp.sin(angles)
    lower_section = values[..., :half_width]
    upper_half = values[..., half_width:]
    return jnp.concatenate([lower_section * cos_part - upper_half * sin_part, upper_half * cos_part + lower_section * sin_part], axis=-1)

def query_positions(lengths, stretch_len):
    remainder = lengths % stretch_len
    return jnp.stack([remainder, remainder + stretch_len, jnp.zeros_like(remainder) + (stretch_len + stretch_len // 2)], axis=-1).astype(jnp.float32)

def reference(query, key_cache, value_cache, new_key, new_value, lengths, out_weight):
    scaling = 1.0 / math.sqrt(HD)

    def one_sequence(per_seq):
        query_one, key_one, value_one, incoming_key, fresh_value, cache_length = per_seq
        query_pos = query_positions(cache_length, STRETCH)
        query_rot = apply_rotary(query_one.astype(jnp.float32)[None], query_pos[:, None]).astype(jnp.bfloat16)
        positions = jnp.arange(CACHE, dtype=jnp.int32)
        key_rot = apply_rotary(key_one.astype(jnp.float32), (positions % STRETCH).astype(jnp.float32)[:, None]).astype(jnp.bfloat16)
        query_by_group = query_rot.astype(jnp.float32).reshape(3, KVH, GROUP, HD)
        scores = jnp.einsum('vkgd,pkd->vkgp', query_by_group, key_rot.astype(jnp.float32)) * scaling
        query_stretch = cache_length // STRETCH
        key_stretch = positions // STRETCH
        key_class = jnp.where(key_stretch == query_stretch, 0, jnp.where(key_stretch == query_stretch - 1, 1, 2))
        selected_branch = jnp.where(key_class == 0, scores[0], jnp.where(key_class == 1, scores[1], scores[2]))
        live_mask = (positions < cache_length).reshape(N_SEQ, POS_DEV)
        blocks = jnp.where(live_mask, selected_branch.reshape(KVH, GROUP, N_SEQ, POS_DEV), NEG_FILL)
        block_max = lax.optimization_barrier(jnp.max(blocks, axis=-1))
        weights = jnp.where(live_mask, jnp.exp(blocks - block_max[..., None]), 0.0)
        block_total = lax.optimization_barrier(jnp.sum(weights, axis=-1))
        block_acc = jnp.einsum('kgnp,npkd->kgnd', weights.astype(jnp.bfloat16).astype(jnp.float32), value_one.astype(jnp.float32).reshape(N_SEQ, POS_DEV, KVH, HD))
        current_key = apply_rotary(incoming_key.astype(jnp.float32), query_pos[0]).astype(jnp.bfloat16)
        self_score = jnp.einsum('kgd,kd->kg', query_by_group[0], current_key.astype(jnp.float32)) * scaling
        top_score = jnp.maximum(self_score, lax.optimization_barrier(jnp.max(block_max, axis=-1)))
        factor = jnp.exp(block_max - top_score[..., None])
        self_factor = jnp.exp(self_score - top_score)
        total = self_factor + lax.optimization_barrier(jnp.sum(block_total * factor, axis=-1))
        accum = fresh_value.astype(jnp.float32)[:, None, :] * self_factor[..., None] + lax.optimization_barrier(jnp.sum(block_acc * factor[..., None], axis=2))
        return (accum / total[..., None]).reshape(HQ, HD).astype(jnp.bfloat16)
    attended = lax.map(one_sequence, (query, key_cache, value_cache, new_key, new_value, lengths))
    return jnp.dot(attended.reshape(B, HQ * HD), out_weight, preferred_element_type=jnp.float32)
```

```python
import functools
import math

import jax
import jax.numpy as jnp
from jax import lax
from jax.experimental import pallas as pl
from jax.experimental.pallas import tpu as pltpu
from jax.sharding import PartitionSpec as P

THETA_BASE = 10000000.0
NEG_FILL = -1e30
SLOT = 16
F32 = jnp.float32
BF16 = jnp.bfloat16


def frequencies(shape):
    width = shape[-1]
    half = width // 2
    lane = lax.broadcasted_iota(jnp.int32, shape, len(shape) - 1)
    index = jnp.where(lane < half, lane, lane - half).astype(F32)
    return jnp.exp(index * F32(-2.0 * math.log(THETA_BASE) / width))


def half_sign(shape):
    lane = lax.broadcasted_iota(jnp.int32, shape, len(shape) - 1)
    return jnp.where(lane < shape[-1] // 2, F32(-1.0), F32(1.0))


def rotate(values, cos_part, signed_sin):
    return values * cos_part + pltpu.roll(values, values.shape[-1] // 2, 1) * signed_sin


def rows_of_scalars(scalars, shape):
    row = lax.broadcasted_iota(jnp.int32, shape, 0)
    out = jnp.zeros(shape, scalars[0].dtype)
    for i, s in enumerate(scalars):
        out = jnp.where(row == i, s, out)
    return out


def attention_kernel(
    lens_ref, place_ref, q_ref, nk_ref, nv_ref, k_hbm, v_hbm,
    out_ref,
    kbuf, vbuf, kcat, qbd, qin, scores, cos_tab, sin_tab, coarse_c, coarse_s, ksem, vsem,
    *, stretch, kv, chunks,
):
    batch, rows, width = kbuf.shape
    heads = q_ref.shape[1]
    group = heads // kv
    lanes = batch * SLOT
    span = rows // kv
    chunk = rows // chunks
    pairs = batch // 2

    def kcopy(c):
        return pltpu.make_async_copy(
            k_hbm.at[:, pl.ds(c * chunk, chunk), :], kbuf.at[:, pl.ds(c * chunk, chunk), :], ksem.at[c]
        )

    def vcopy(c):
        return pltpu.make_async_copy(
            v_hbm.at[pl.ds(2 * c, 2)], vbuf.at[pl.ds(2 * c, 2)], vsem.at[c]
        )

    for c in range(chunks):
        kcopy(c).start()
    for c in range(pairs):
        vcopy(c).start()

    place = place_ref[0]
    base = place * span
    key_stretch = base // stretch

    freq8 = frequencies((8, width))
    sign8 = half_sign((8, width))
    row8 = lax.broadcasted_iota(jnp.int32, (8, width), 0)
    per8 = 8 // kv
    fine = (row8 // kv).astype(F32) * freq8
    fine_c, fine_s = jnp.cos(fine), jnp.sin(fine) * sign8
    n8 = rows // 8
    start = (base % stretch).astype(F32)
    coarse_pos = start + (lax.broadcasted_iota(jnp.int32, (n8, width), 0) * per8).astype(F32)
    coarse = coarse_pos * frequencies((n8, width))
    coarse_c[...] = jnp.cos(coarse)
    coarse_s[...] = jnp.sin(coarse) * half_sign((n8, width))

    def table(i, carry):
        cc = coarse_c[pl.ds(i, 1), :]
        cs = coarse_s[pl.ds(i, 1), :]
        cos_tab[pl.ds(pl.multiple_of(i * 8, 8), 8), :] = cc * fine_c - cs * fine_s
        sin_tab[pl.ds(pl.multiple_of(i * 8, 8), 8), :] = cs * fine_c + cc * fine_s
        return carry

    lax.fori_loop(0, n8, table, 0, unroll=8)

    picked, intra, limit = [], [], []
    for b in range(batch):
        p = lens_ref[b]
        qc = p // stretch
        r = p - qc * stretch
        intra.append(r.astype(F32))
        inter = stretch + stretch // 2
        picked.append(
            jnp.where(key_stretch == qc, r, jnp.where(key_stretch == qc - 1, r + stretch, inter)).astype(F32)
        )
        limit.append((p - base) * kv)
    angle_p = rows_of_scalars(picked, (8, width)) * freq8
    angle_r = rows_of_scalars(intra, (8, width)) * freq8
    cp, sp = jnp.cos(angle_p), jnp.sin(angle_p) * sign8
    cr, sr = jnp.cos(angle_r), jnp.sin(angle_r) * sign8

    qbd[...] = jnp.zeros_like(qbd)
    qin[...] = jnp.zeros_like(qin)
    for b in range(batch):
        q = q_ref[b].astype(F32)
        qbd[b * SLOT : b * SLOT + heads, b * width : (b + 1) * width] = rotate(
            q, cp[b : b + 1], sp[b : b + 1]
        ).astype(BF16)
        qin[b * SLOT : b * SLOT + heads, :] = rotate(q, cr[b : b + 1], sr[b : b + 1]).astype(BF16)

    scaling = F32(1.0 / math.sqrt(width))

    own_rows = batch * kv
    knew = jnp.concatenate(
        [rotate(nk_ref[b].astype(F32), cr[b : b + 1], sr[b : b + 1]) for b in range(batch)], axis=0
    ).astype(BF16)
    own_all = lax.dot_general(
        knew, qin[...], (((1,), (1,)), ((), ())), preferred_element_type=F32
    ) * scaling
    own_row = lax.broadcasted_iota(jnp.int32, (own_rows, lanes), 0)
    own_lane = lax.broadcasted_iota(jnp.int32, (own_rows, lanes), 1)
    own_kv = jnp.minimum((own_lane % SLOT) // group, kv - 1)
    own_mask = (own_row // kv == own_lane // SLOT) & (own_row % kv == own_kv)
    own = jnp.sum(jnp.where(own_mask, own_all, 0.0), axis=0, keepdims=True)
    first = place == 0
    own = jnp.where(first, own, F32(NEG_FILL))

    lane1 = lax.broadcasted_iota(jnp.int32, (1, lanes), 1)
    bound = jnp.zeros((1, lanes), jnp.int32)
    for b in range(batch):
        bound = jnp.where(lane1 // SLOT == b, limit[b], bound)
    lane_kv = jnp.minimum((lane1 % SLOT) // group, kv - 1)
    row_c = lax.broadcasted_iota(jnp.int32, (chunk, lanes), 0)
    fits = row_c % kv == lane_kv

    top = own
    for c in range(chunks):
        kcopy(c).wait()

        def turn(i, carry):
            at = pl.multiple_of(i * 64, 64)
            cc = cos_tab[pl.ds(c * chunk + at, 64), :]
            ss = sin_tab[pl.ds(c * chunk + at, 64), :]
            for b in range(batch):
                k = kbuf[b, pl.ds(c * chunk + at, 64), :].astype(F32)
                kcat[pl.ds(at, 64), b * width : (b + 1) * width] = rotate(k, cc, ss).astype(BF16)
            return carry

        lax.fori_loop(0, chunk // 64, turn, 0)
        s = lax.dot_general(
            kcat[...], qbd[...], (((1,), (1,)), ((), ())), preferred_element_type=F32
        ) * scaling
        s = jnp.where(fits & (row_c + c * chunk < bound), s, F32(NEG_FILL))
        scores[c * chunk : (c + 1) * chunk, :] = s
        top = jnp.maximum(top, jnp.max(s, axis=0, keepdims=True))

    own_w = jnp.where(first, jnp.exp(own - top), 0.0)
    total = own_w
    parts = []
    for c in range(chunks):
        s = scores[c * chunk : (c + 1) * chunk, :]
        w = jnp.where(s > F32(0.5 * NEG_FILL), jnp.exp(s - top), 0.0)
        total = total + jnp.sum(w, axis=0, keepdims=True)
        parts.append(jnp.transpose(w.astype(BF16)))
    wt = jnp.concatenate(parts, axis=1)

    own_wt = jnp.transpose(jnp.where(own_mask, own_w, 0.0))
    nv = jnp.concatenate([nv_ref[b].astype(F32) for b in range(batch)], axis=0)
    own_acc = lax.dot_general(
        own_wt, nv, (((1,), (0,)), ((), ())), preferred_element_type=F32,
        precision=lax.Precision.HIGHEST,
    )

    for c in range(pairs):
        vcopy(c).wait()
        v = jnp.concatenate([vbuf[2 * c], vbuf[2 * c + 1]], axis=1)
        acc = jnp.dot(wt[2 * c * SLOT : (2 * c + 2) * SLOT, :], v, preferred_element_type=F32)
        for j in range(2):
            b = 2 * c + j
            part = acc[j * SLOT : (j + 1) * SLOT, j * width : (j + 1) * width]
            part = part + own_acc[b * SLOT : (b + 1) * SLOT, :]
            out_ref[pl.ds(b, heads, stride=batch), :] = part[:heads]

    lane_b = lax.broadcasted_iota(jnp.int32, (batch, lanes), 1)
    row_b = lax.broadcasted_iota(jnp.int32, (batch, lanes), 0)
    stats = jnp.zeros((batch, lanes), F32)
    for b in range(batch):
        m_b = pltpu.roll(top, (lanes - b * SLOT) % lanes, 1) if b else top
        l_b = pltpu.roll(total, (lanes + SLOT - b * SLOT) % lanes, 1) if b != 1 else total
        stats = jnp.where(row_b == b, jnp.where(lane_b < SLOT, m_b, l_b), stats)
    out_ref[heads * batch :, :] = stats


def merge(a_ref, b_ref, heads, batch):
    a = a_ref[heads * batch :, :]
    b = b_ref[heads * batch :, :]
    top = jnp.maximum(a, b)
    fa, fb = jnp.exp(a - top), jnp.exp(b - top)
    total = a * pltpu.roll(fa, SLOT, 1) + b * pltpu.roll(fb, SLOT, 1)
    lane = lax.broadcasted_iota(jnp.int32, top.shape, 1)
    stats = jnp.where(lane < SLOT, top, total)
    sums = []
    for h in range(heads):
        rows = slice(h * batch, (h + 1) * batch)
        sums.append(a_ref[rows, :] * fa[:, h : h + 1] + b_ref[rows, :] * fb[:, h : h + 1])
    return sums, stats


def merge_kernel(a_ref, b_ref, out_ref, *, heads, batch):
    sums, stats = merge(a_ref, b_ref, heads, batch)
    for h in range(heads):
        out_ref[h * batch : (h + 1) * batch, :] = sums[h]
    out_ref[heads * batch :, :] = stats


def project_kernel(a_ref, b_ref, w_ref, out_ref, *, heads, batch):
    sums, stats = merge(a_ref, b_ref, heads, batch)
    attended = jnp.concatenate(
        [(sums[h] / stats[:, SLOT + h : SLOT + h + 1]).astype(BF16) for h in range(heads)], axis=1
    )
    out_ref[...] = jnp.dot(attended, w_ref[...], preferred_element_type=F32)


def in_vmem(count):
    return [pl.BlockSpec(memory_space=pltpu.VMEM)] * count


def butterfly(values, axis):
    size = lax.axis_size(axis)
    assert size & (size - 1) == 0
    return [[(i, i ^ (1 << k)) for i in range(size)] for k in range(size.bit_length() - 1)]


def body(query, key_cache, value_cache, new_key, new_value, lengths, out_weight):
    seq_count = lax.axis_size("seq")
    batch, span, kv, width = key_cache.shape
    heads = query.shape[1]
    stretch = span * seq_count // 8
    rows = span * kv
    chunks = 4
    lanes = batch * SLOT
    place = lax.axis_index("seq").astype(jnp.int32).reshape(1)
    packed_rows = heads * batch + batch
    any_space = pl.BlockSpec(memory_space=pl.ANY)
    smem = pl.BlockSpec(memory_space=pltpu.SMEM)
    packed = pl.pallas_call(
        functools.partial(attention_kernel, stretch=stretch, kv=kv, chunks=chunks),
        out_shape=jax.ShapeDtypeStruct((packed_rows, width), F32),
        in_specs=[smem, smem] + in_vmem(3) + [any_space, any_space],
        out_specs=pl.BlockSpec(memory_space=pltpu.VMEM),
        scratch_shapes=[
            pltpu.VMEM((batch, rows, width), BF16),
            pltpu.VMEM((batch, rows, width), BF16),
            pltpu.VMEM((rows // chunks, batch * width), BF16),
            pltpu.VMEM((lanes, batch * width), BF16),
            pltpu.VMEM((lanes, width), BF16),
            pltpu.VMEM((rows, lanes), F32),
            pltpu.VMEM((rows, width), F32),
            pltpu.VMEM((rows, width), F32),
            pltpu.VMEM((rows // 8, width), F32),
            pltpu.VMEM((rows // 8, width), F32),
            pltpu.SemaphoreType.DMA((chunks,)),
            pltpu.SemaphoreType.DMA((batch // 2,)),
        ],
        name="attention",
    )(
        lengths, place, query, new_key, new_value,
        key_cache.reshape(batch, rows, width), value_cache.reshape(batch, rows, width),
    )
    steps = butterfly(packed, "seq")
    for pairs in steps[:-1]:
        other = lax.ppermute(packed, "seq", pairs)
        packed = pl.pallas_call(
            functools.partial(merge_kernel, heads=heads, batch=batch),
            out_shape=jax.ShapeDtypeStruct(packed.shape, F32),
            in_specs=in_vmem(2),
            out_specs=pl.BlockSpec(memory_space=pltpu.VMEM),
            name="merge",
        )(packed, other)
    other = lax.ppermute(packed, "seq", steps[-1])
    partial_out = pl.pallas_call(
        functools.partial(project_kernel, heads=heads, batch=batch),
        out_shape=jax.ShapeDtypeStruct((batch, out_weight.shape[1]), F32),
        in_specs=in_vmem(3),
        out_specs=pl.BlockSpec(memory_space=pltpu.VMEM),
        name="project",
    )(packed, other, out_weight)
    for pairs in reversed(butterfly(partial_out, "head")):
        partial_out = partial_out + lax.ppermute(partial_out, "head", pairs)
    return partial_out


def solution(mesh):
    placed = (
        P(None, "head", None),
        P(None, "seq", "head", None),
        P(None, "seq", "head", None),
        P(None, "head", None),
        P(None, "head", None),
        P(),
        P("head", "seq"),
    )
    return jax.shard_map(
        body, mesh=mesh, in_specs=placed, out_specs=P(None, "seq"), check_vma=False
    )
```

```python
import functools
import math

import jax
import jax.numpy as jnp
from jax import lax
from jax.experimental import pallas as pl
from jax.experimental.pallas import tpu as pltpu
from jax.sharding import PartitionSpec as P
import numpy as np

THETA_BASE = 10000000.0
NEG_FILL = -1e30
SLOT = 16
F32 = jnp.float32
BF16 = jnp.bfloat16


def frequencies(shape):
    width = shape[-1]
    half = width // 2
    lane = lax.broadcasted_iota(jnp.int32, shape, len(shape) - 1)
    index = jnp.where(lane < half, lane, lane - half).astype(F32)
    return jnp.exp(index * F32(-2.0 * math.log(THETA_BASE) / width))


def half_sign(shape):
    lane = lax.broadcasted_iota(jnp.int32, shape, len(shape) - 1)
    return jnp.where(lane < shape[-1] // 2, F32(-1.0), F32(1.0))


def rotate(values, cos_part, signed_sin):
    return values * cos_part + pltpu.roll(values, values.shape[-1] // 2, 1) * signed_sin


def rows_of_scalars(scalars, shape):
    row = lax.broadcasted_iota(jnp.int32, shape, 0)
    out = jnp.zeros(shape, scalars[0].dtype)
    for i, s in enumerate(scalars):
        out = jnp.where(row == i, s, out)
    return out


def attention_kernel(
    tab_hbm, lens_hbm, q_hbm, nk_hbm, nv_hbm, k_hbm, v_hbm,
    out_ref,
    tab, lens, qbuf, nkbuf, nvbuf, kbuf, vbuf, kcat0, kcat1, qbd, qin, qrot, scores,
    tsem, ksem, vsem, lsem, qsem, nksem, nvsem,
    *, stretch, kv, chunks,
):
    batch, rows, width = kbuf.shape
    heads = qbuf.shape[0]
    group = heads // kv
    lanes = batch * SLOT
    span = rows // kv
    chunk = rows // chunks
    pairs = batch // 2
    whole_stretch = span == stretch
    kcats = (kcat0, kcat1)

    def tcopy(c):
        part = pl.ds(c * chunk, chunk)
        return pltpu.make_async_copy(tab_hbm.at[:, part, :], tab.at[:, part, :], tsem.at[c])

    def kcopy(c):
        part = pl.ds(c * chunk, chunk)
        return pltpu.make_async_copy(k_hbm.at[:, part, :], kbuf.at[:, part, :], ksem.at[c])

    def vcopy(c):
        part = pl.ds(2 * c, 2)
        return pltpu.make_async_copy(v_hbm.at[part], vbuf.at[part], vsem.at[c])

    lcopy = pltpu.make_async_copy(lens_hbm, lens, lsem)
    qcopy = pltpu.make_async_copy(q_hbm, qbuf, qsem)
    nkcopy = pltpu.make_async_copy(nk_hbm, nkbuf, nksem)
    nvcopy = pltpu.make_async_copy(nv_hbm, nvbuf, nvsem)
    lcopy.start()
    qcopy.start()
    nkcopy.start()
    for c in range(chunks):
        if whole_stretch:
            tcopy(c).start()
        kcopy(c).start()
    nvcopy.start()
    for c in range(pairs):
        vcopy(c).start()

    place = lax.axis_index("seq").astype(jnp.int32)
    base = place * span
    key_stretch = base // stretch

    qbd[...] = jnp.zeros_like(qbd)
    qin[...] = jnp.zeros_like(qin)
    freq8 = frequencies((batch, width))
    sign8 = half_sign((batch, width))
    if not whole_stretch:
        row = lax.broadcasted_iota(jnp.int32, (rows, width), 0)
        angle = (base % stretch + row // kv).astype(F32) * frequencies((rows, width))
        tab[0] = jnp.cos(angle)
        tab[1] = jnp.sin(angle) * half_sign((rows, width))

    lcopy.wait()
    picked, intra, limit = [], [], []
    for b in range(batch):
        p = lens[b]
        qc = p // stretch
        r = p - qc * stretch
        intra.append(r.astype(F32))
        inter = stretch + stretch // 2
        picked.append(
            jnp.where(key_stretch == qc, r, jnp.where(key_stretch == qc - 1, r + stretch, inter)).astype(F32)
        )
        limit.append((p - base) * kv)
    angle_p = rows_of_scalars(picked, (batch, width)) * freq8
    angle_r = rows_of_scalars(intra, (batch, width)) * freq8
    cp, sp = jnp.cos(angle_p), jnp.sin(angle_p) * sign8
    cr, sr = jnp.cos(angle_r), jnp.sin(angle_r) * sign8

    qcopy.wait()
    for h in range(heads):
        q = qbuf[h].astype(F32)
        at = slice(h * batch, (h + 1) * batch)
        qrot[0, at, :] = rotate(q, cp, sp)
        qrot[1, at, :] = rotate(q, cr, sr)
    for b in range(batch):
        mine = pl.ds(b, heads, stride=batch)
        at = slice(b * SLOT, b * SLOT + heads)
        qbd[at, b * width : (b + 1) * width] = qrot[0, mine, :].astype(BF16)
        qin[at, :] = qrot[1, mine, :].astype(BF16)

    scaling = F32(1.0 / math.sqrt(width))

    own_rows = batch * kv
    nkcopy.wait()
    knew = jnp.concatenate(
        [rotate(nkbuf[b].astype(F32), cr[b : b + 1], sr[b : b + 1]) for b in range(batch)], axis=0
    ).astype(BF16)
    own_all = lax.dot_general(
        knew, qin[...], (((1,), (1,)), ((), ())), preferred_element_type=F32
    ) * scaling
    own_row = lax.broadcasted_iota(jnp.int32, (own_rows, lanes), 0)
    own_lane = lax.broadcasted_iota(jnp.int32, (own_rows, lanes), 1)
    own_kv = jnp.minimum((own_lane % SLOT) // group, kv - 1)
    own_mask = (own_row // kv == own_lane // SLOT) & (own_row % kv == own_kv)
    own = jnp.sum(jnp.where(own_mask, own_all, 0.0), axis=0, keepdims=True)
    first = place == 0
    own = jnp.where(first, own, F32(NEG_FILL))

    lane1 = lax.broadcasted_iota(jnp.int32, (1, lanes), 1)
    bound = jnp.zeros((1, lanes), jnp.int32)
    for b in range(batch):
        bound = jnp.where(lane1 // SLOT == b, limit[b], bound)
    lane_kv = jnp.minimum((lane1 % SLOT) // group, kv - 1)
    row_c = lax.broadcasted_iota(jnp.int32, (chunk, lanes), 0)
    fits = row_c % kv == lane_kv

    def rotate_keys(c):
        part = slice(c * chunk, (c + 1) * chunk)
        for b in range(batch):
            k = kbuf[b, part, :].astype(F32)
            kcats[c % 2][:, b * width : (b + 1) * width] = rotate(k, tab[0, part, :], tab[1, part, :]).astype(BF16)

    def score(c, top):
        s = lax.dot_general(
            kcats[c % 2][...], qbd[...], (((1,), (1,)), ((), ())), preferred_element_type=F32
        ) * scaling
        s = jnp.where(fits & (row_c + c * chunk < bound), s, F32(NEG_FILL))
        scores[c * chunk : (c + 1) * chunk, :] = s
        return jnp.maximum(top, jnp.max(s, axis=0, keepdims=True))

    top = own
    for c in range(chunks):
        if whole_stretch:
            tcopy(c).wait()
        kcopy(c).wait()
        rotate_keys(c)
        if c:
            top = score(c - 1, top)
    top = score(chunks - 1, top)

    own_w = jnp.where(first, jnp.exp(own - top), 0.0)
    total = own_w
    parts = []
    for c in range(chunks):
        s = scores[c * chunk : (c + 1) * chunk, :]
        w = jnp.where(s > F32(0.5 * NEG_FILL), jnp.exp(s - top), 0.0)
        total = total + jnp.sum(w, axis=0, keepdims=True)
        parts.append(jnp.transpose(w.astype(BF16)))
    wt = jnp.concatenate(parts, axis=1)

    nvcopy.wait()
    own_wt = jnp.transpose(jnp.where(own_mask, own_w, 0.0))
    nv = jnp.concatenate([nvbuf[b].astype(F32) for b in range(batch)], axis=0)
    own_acc = lax.dot_general(
        own_wt, nv, (((1,), (0,)), ((), ())), preferred_element_type=F32,
        precision=lax.Precision.HIGHEST,
    )

    for c in range(pairs):
        vcopy(c).wait()
        v = jnp.concatenate([vbuf[2 * c], vbuf[2 * c + 1]], axis=1)
        acc = jnp.dot(wt[2 * c * SLOT : (2 * c + 2) * SLOT, :], v, preferred_element_type=F32)
        for j in range(2):
            b = 2 * c + j
            part = acc[j * SLOT : (j + 1) * SLOT, j * width : (j + 1) * width]
            part = part + own_acc[b * SLOT : (b + 1) * SLOT, :]
            out_ref[pl.ds(b, heads, stride=batch), :] = part[:heads]

    lane_b = lax.broadcasted_iota(jnp.int32, (batch, lanes), 1)
    row_b = lax.broadcasted_iota(jnp.int32, (batch, lanes), 0)
    stats = jnp.zeros((batch, lanes), F32)
    for b in range(batch):
        m_b = pltpu.roll(top, (lanes - b * SLOT) % lanes, 1) if b else top
        l_b = pltpu.roll(total, (lanes + SLOT - b * SLOT) % lanes, 1) if b != 1 else total
        stats = jnp.where(row_b == b, jnp.where(lane_b < SLOT, m_b, l_b), stats)
    out_ref[heads * batch :, :] = stats


def merge(a_ref, b_ref, heads, batch):
    a = a_ref[heads * batch :, :]
    b = b_ref[heads * batch :, :]
    top = jnp.maximum(a, b)
    fa, fb = jnp.exp(a - top), jnp.exp(b - top)
    total = a * pltpu.roll(fa, SLOT, 1) + b * pltpu.roll(fb, SLOT, 1)
    lane = lax.broadcasted_iota(jnp.int32, top.shape, 1)
    stats = jnp.where(lane < SLOT, top, total)
    sums = []
    for h in range(heads):
        rows = slice(h * batch, (h + 1) * batch)
        sums.append(a_ref[rows, :] * fa[:, h : h + 1] + b_ref[rows, :] * fb[:, h : h + 1])
    return sums, stats


def merge_kernel(a_ref, b_ref, out_ref, *, heads, batch):
    sums, stats = merge(a_ref, b_ref, heads, batch)
    for h in range(heads):
        out_ref[h * batch : (h + 1) * batch, :] = sums[h]
    out_ref[heads * batch :, :] = stats


def project_kernel(a_ref, b_ref, w_ref, out_ref, *, heads, batch):
    sums, stats = merge(a_ref, b_ref, heads, batch)
    attended = jnp.concatenate(
        [(sums[h] / stats[:, SLOT + h : SLOT + h + 1]).astype(BF16) for h in range(heads)], axis=1
    )
    out_ref[...] = jnp.dot(attended, w_ref[...], preferred_element_type=F32)


def vmem(x):
    return pltpu.with_memory_space_constraint(x, pltpu.VMEM)


def in_vmem(count):
    return [pl.BlockSpec(memory_space=pltpu.VMEM)] * count


def butterfly(axis):
    size = lax.axis_size(axis)
    assert size & (size - 1) == 0
    return [[(i, i ^ (1 << k)) for i in range(size)] for k in range(size.bit_length() - 1)]


def rope_tables(span, kv, width):
    half = width // 2
    index = np.arange(half, dtype=np.float32)
    freq = np.exp(index * np.float32(-2.0 * math.log(THETA_BASE) / width)).astype(np.float32)
    angle = np.arange(span, dtype=np.float32)[:, None] * freq
    cos_part, sin_part = np.cos(angle.astype(np.float64)), np.sin(angle.astype(np.float64))
    both = np.stack([np.concatenate([cos_part, cos_part], 1), np.concatenate([-sin_part, sin_part], 1)])
    return np.repeat(both, kv, axis=1).astype(np.float32)


def body(query, key_cache, value_cache, new_key, new_value, lengths, out_weight):
    seq_count = lax.axis_size("seq")
    batch, span, kv, width = key_cache.shape
    heads = query.shape[1]
    stretch = span * seq_count // 8
    rows = span * kv
    chunks = 4
    lanes = batch * SLOT
    packed_rows = heads * batch + batch
    if span == stretch:
        tables = jnp.asarray(rope_tables(span, kv, width))
    else:
        tables = jnp.zeros((2, 8, width), F32)
    dma = pltpu.SemaphoreType.DMA
    packed = pl.pallas_call(
        functools.partial(attention_kernel, stretch=stretch, kv=kv, chunks=chunks),
        out_shape=pltpu.VMEM((packed_rows, width), F32),
        in_specs=[pl.BlockSpec(memory_space=pl.ANY)] * 7,
        out_specs=pl.BlockSpec(memory_space=pltpu.VMEM),
        scratch_shapes=[
            pltpu.VMEM((2, rows, width), F32),
            pltpu.SMEM((batch,), jnp.int32),
            pltpu.VMEM((heads, batch, width), BF16),
            pltpu.VMEM((batch, kv, width), BF16),
            pltpu.VMEM((batch, kv, width), BF16),
            pltpu.VMEM((batch, rows, width), BF16),
            pltpu.VMEM((batch, rows, width), BF16),
            pltpu.VMEM((rows // chunks, batch * width), BF16),
            pltpu.VMEM((rows // chunks, batch * width), BF16),
            pltpu.VMEM((lanes, batch * width), BF16),
            pltpu.VMEM((lanes, width), BF16),
            pltpu.VMEM((2, heads * batch, width), F32),
            pltpu.VMEM((rows, lanes), F32),
            dma((chunks,)), dma((chunks,)), dma((batch // 2,)), dma, dma, dma, dma,
        ],
        name="attention",
    )(
        tables, lengths, jnp.transpose(query, (1, 0, 2)), new_key, new_value,
        key_cache.reshape(batch, rows, width), value_cache.reshape(batch, rows, width),
    )
    steps = butterfly("seq")
    for pairs in steps[:-1]:
        other = lax.ppermute(packed, "seq", pairs)
        packed = pl.pallas_call(
            functools.partial(merge_kernel, heads=heads, batch=batch),
            out_shape=pltpu.VMEM(packed.shape, F32),
            in_specs=in_vmem(2),
            out_specs=pl.BlockSpec(memory_space=pltpu.VMEM),
            name="merge",
        )(vmem(packed), vmem(other))
    other = lax.ppermute(packed, "seq", steps[-1])
    share = pl.pallas_call(
        functools.partial(project_kernel, heads=heads, batch=batch),
        out_shape=pltpu.VMEM((batch, out_weight.shape[1]), F32),
        in_specs=in_vmem(3),
        out_specs=pl.BlockSpec(memory_space=pltpu.VMEM),
        name="project",
    )(vmem(packed), vmem(other), vmem(out_weight))
    for pairs in reversed(butterfly("head")):
        share = share + lax.ppermute(share, "head", pairs)
    return share


def solution(mesh):
    placed = (
        P(None, "head", None),
        P(None, "seq", "head", None),
        P(None, "seq", "head", None),
        P(None, "head", None),
        P(None, "head", None),
        P(),
        P("head", "seq"),
    )
    return jax.shard_map(
        body, mesh=mesh, in_specs=placed, out_specs=P(None, "seq"), check_vma=False
    )
```

```python
import functools
import math

import jax
import jax.numpy as jnp
from jax import lax
from jax.experimental import pallas as pl
from jax.experimental.pallas import tpu as pltpu
from jax.sharding import PartitionSpec as P
import numpy as np

THETA_BASE = 10000000.0
NEG_FILL = -1e30
SLOT = 16
F32 = jnp.float32
BF16 = jnp.bfloat16


def frequencies(shape):
    width = shape[-1]
    half = width // 2
    lane = lax.broadcasted_iota(jnp.int32, shape, len(shape) - 1)
    index = jnp.where(lane < half, lane, lane - half).astype(F32)
    return jnp.exp(index * F32(-2.0 * math.log(THETA_BASE) / width))


def half_sign(shape):
    lane = lax.broadcasted_iota(jnp.int32, shape, len(shape) - 1)
    return jnp.where(lane < shape[-1] // 2, F32(-1.0), F32(1.0))


def rotate(values, cos_part, signed_sin):
    return values * cos_part + pltpu.roll(values, values.shape[-1] // 2, 1) * signed_sin


def rows_of_scalars(scalars, shape):
    row = lax.broadcasted_iota(jnp.int32, shape, 0)
    out = jnp.zeros(shape, scalars[0].dtype)
    for i, s in enumerate(scalars):
        out = jnp.where(row == i, s, out)
    return out


def attention_kernel(
    tab_hbm, lens_hbm, q_hbm, nk_hbm, nv_hbm, k_hbm, v_hbm, w_hbm,
    out_ref, w_ref,
    tab, lens, qbuf, nkbuf, nvbuf, kbuf, vbuf, kcat0, kcat1, qbd, qin, qrot, scores,
    tsem, ksem, vsem, lsem, qsem, nksem, nvsem, wsem,
    *, stretch, kv, chunks,
):
    batch, rows, width = kbuf.shape
    heads = qbuf.shape[0]
    group = heads // kv
    lanes = batch * SLOT
    span = rows // kv
    chunk = rows // chunks
    pairs = batch // 2
    whole_stretch = span == stretch
    kcats = (kcat0, kcat1)

    def tcopy(c):
        part = pl.ds(c * chunk, chunk)
        return pltpu.make_async_copy(tab_hbm.at[:, part, :], tab.at[:, part, :], tsem.at[c])

    def kcopy(c):
        part = pl.ds(c * chunk, chunk)
        return pltpu.make_async_copy(k_hbm.at[:, part, :], kbuf.at[:, part, :], ksem.at[c])

    def vcopy(c):
        part = pl.ds(2 * c, 2)
        return pltpu.make_async_copy(v_hbm.at[part], vbuf.at[part], vsem.at[c])

    wcopy = pltpu.make_async_copy(w_hbm, w_ref, wsem)

    lcopy = pltpu.make_async_copy(lens_hbm, lens, lsem)
    qcopy = pltpu.make_async_copy(q_hbm, qbuf, qsem)
    nkcopy = pltpu.make_async_copy(nk_hbm, nkbuf, nksem)
    nvcopy = pltpu.make_async_copy(nv_hbm, nvbuf, nvsem)
    lcopy.start()
    qcopy.start()
    nkcopy.start()
    for c in range(chunks):
        if whole_stretch:
            tcopy(c).start()
        kcopy(c).start()
    nvcopy.start()

    place = lax.axis_index("seq").astype(jnp.int32)
    base = place * span
    key_stretch = base // stretch

    qbd[...] = jnp.zeros_like(qbd)
    qin[...] = jnp.zeros_like(qin)
    freq8 = frequencies((batch, width))
    sign8 = half_sign((batch, width))
    if not whole_stretch:
        row = lax.broadcasted_iota(jnp.int32, (rows, width), 0)
        angle = (base % stretch + row // kv).astype(F32) * frequencies((rows, width))
        tab[0] = jnp.cos(angle)
        tab[1] = jnp.sin(angle) * half_sign((rows, width))

    lcopy.wait()
    picked, intra, limit = [], [], []
    for b in range(batch):
        p = lens[b]
        qc = p // stretch
        r = p - qc * stretch
        intra.append(r.astype(F32))
        inter = stretch + stretch // 2
        picked.append(
            jnp.where(key_stretch == qc, r, jnp.where(key_stretch == qc - 1, r + stretch, inter)).astype(F32)
        )
        limit.append((p - base) * kv)
    angle_p = rows_of_scalars(picked, (batch, width)) * freq8
    angle_r = rows_of_scalars(intra, (batch, width)) * freq8
    cp, sp = jnp.cos(angle_p), jnp.sin(angle_p) * sign8
    cr, sr = jnp.cos(angle_r), jnp.sin(angle_r) * sign8

    qcopy.wait()
    for h in range(heads):
        q = qbuf[h].astype(F32)
        at = slice(h * batch, (h + 1) * batch)
        qrot[0, at, :] = rotate(q, cp, sp)
        qrot[1, at, :] = rotate(q, cr, sr)
    for b in range(batch):
        mine = pl.ds(b, heads, stride=batch)
        at = slice(b * SLOT, b * SLOT + heads)
        qbd[at, b * width : (b + 1) * width] = qrot[0, mine, :].astype(BF16)
        qin[at, :] = qrot[1, mine, :].astype(BF16)

    scaling = F32(1.0 / math.sqrt(width))

    own_rows = batch * kv
    nkcopy.wait()
    knew = jnp.concatenate(
        [rotate(nkbuf[b].astype(F32), cr[b : b + 1], sr[b : b + 1]) for b in range(batch)], axis=0
    ).astype(BF16)
    own_all = lax.dot_general(
        knew, qin[...], (((1,), (1,)), ((), ())), preferred_element_type=F32
    ) * scaling
    own_row = lax.broadcasted_iota(jnp.int32, (own_rows, lanes), 0)
    own_lane = lax.broadcasted_iota(jnp.int32, (own_rows, lanes), 1)
    own_kv = jnp.minimum((own_lane % SLOT) // group, kv - 1)
    own_mask = (own_row // kv == own_lane // SLOT) & (own_row % kv == own_kv)
    own = jnp.sum(jnp.where(own_mask, own_all, 0.0), axis=0, keepdims=True)
    first = place == 0
    own = jnp.where(first, own, F32(NEG_FILL))

    lane1 = lax.broadcasted_iota(jnp.int32, (1, lanes), 1)
    bound = jnp.zeros((1, lanes), jnp.int32)
    for b in range(batch):
        bound = jnp.where(lane1 // SLOT == b, limit[b], bound)
    lane_kv = jnp.minimum((lane1 % SLOT) // group, kv - 1)
    row_c = lax.broadcasted_iota(jnp.int32, (chunk, lanes), 0)
    fits = row_c % kv == lane_kv

    def rotate_keys(c):
        part = slice(c * chunk, (c + 1) * chunk)
        for b in range(batch):
            k = kbuf[b, part, :].astype(F32)
            kcats[c % 2][b] = rotate(k, tab[0, part, :], tab[1, part, :]).astype(BF16)

    def score(c, top):
        keys = jnp.concatenate([kcats[c % 2][b] for b in range(batch)], axis=1)
        s = lax.dot_general(
            keys, qbd[...], (((1,), (1,)), ((), ())), preferred_element_type=F32
        ) * scaling
        s = jnp.where(fits & (row_c + c * chunk < bound), s, F32(NEG_FILL))
        scores[c * chunk : (c + 1) * chunk, :] = s
        return jnp.maximum(top, jnp.max(s, axis=0, keepdims=True))

    top = own
    for c in range(chunks):
        if whole_stretch:
            tcopy(c).wait()
        kcopy(c).wait()
        if c == 0:
            for i in range(pairs):
                vcopy(i).start()
        if c == chunks - 1:
            wcopy.start()
        rotate_keys(c)
        if c:
            top = score(c - 1, top)
    top = score(chunks - 1, top)

    own_w = jnp.where(first, jnp.exp(own - top), 0.0)
    total = own_w
    parts = []
    for c in range(chunks):
        s = scores[c * chunk : (c + 1) * chunk, :]
        w = jnp.where(s > F32(0.5 * NEG_FILL), jnp.exp(s - top), 0.0)
        total = total + jnp.sum(w, axis=0, keepdims=True)
        parts.append(jnp.transpose(w.astype(BF16)))
    wt = jnp.concatenate(parts, axis=1)

    nvcopy.wait()
    own_wt = jnp.transpose(jnp.where(own_mask, own_w, 0.0))
    nv = jnp.concatenate([nvbuf[b].astype(F32) for b in range(batch)], axis=0)
    own_acc = lax.dot_general(
        own_wt, nv, (((1,), (0,)), ((), ())), preferred_element_type=F32,
        precision=lax.Precision.HIGHEST,
    )

    for c in range(pairs):
        vcopy(c).wait()
    for c in range(pairs):
        v = jnp.concatenate([vbuf[2 * c], vbuf[2 * c + 1]], axis=1)
        acc = jnp.dot(wt[2 * c * SLOT : (2 * c + 2) * SLOT, :], v, preferred_element_type=F32)
        for j in range(2):
            b = 2 * c + j
            part = acc[j * SLOT : (j + 1) * SLOT, j * width : (j + 1) * width]
            part = part + own_acc[b * SLOT : (b + 1) * SLOT, :]
            out_ref[pl.ds(b, heads, stride=batch), :] = part[:heads]

    lane_b = lax.broadcasted_iota(jnp.int32, (batch, lanes), 1)
    row_b = lax.broadcasted_iota(jnp.int32, (batch, lanes), 0)
    stats = jnp.zeros((batch, lanes), F32)
    for b in range(batch):
        m_b = pltpu.roll(top, (lanes - b * SLOT) % lanes, 1) if b else top
        l_b = pltpu.roll(total, (lanes + SLOT - b * SLOT) % lanes, 1) if b != 1 else total
        stats = jnp.where(row_b == b, jnp.where(lane_b < SLOT, m_b, l_b), stats)
    out_ref[heads * batch :, :] = stats
    wcopy.wait()


def balanced_sum(values):
    while len(values) > 1:
        values = [values[i] + values[i + 1] for i in range(0, len(values), 2)]
    return values[0]


def merge(parts, heads, batch):
    stats = [p[heads * batch :, :] for p in parts]
    top = functools.reduce(jnp.maximum, stats)
    factors = [jnp.exp(s - top) for s in stats]
    total = balanced_sum([s * pltpu.roll(f, SLOT, 1) for s, f in zip(stats, factors)])
    lane = lax.broadcasted_iota(jnp.int32, top.shape, 1)
    sums = []
    for h in range(heads):
        rows = slice(h * batch, (h + 1) * batch)
        sums.append(balanced_sum([p[rows, :] * f[:, h : h + 1] for p, f in zip(parts, factors)]))
    return sums, jnp.where(lane < SLOT, top, total)


def merge_kernel(*refs, heads, batch):
    out_ref = refs[-1]
    sums, stats = merge(refs[:-1], heads, batch)
    for h in range(heads):
        out_ref[h * batch : (h + 1) * batch, :] = sums[h]
    out_ref[heads * batch :, :] = stats


def project_kernel(*refs, heads, batch):
    w_ref, out_ref = refs[-2:]
    sums, stats = merge(refs[:-2], heads, batch)
    attended = jnp.concatenate(
        [(sums[h] / stats[:, SLOT + h : SLOT + h + 1]).astype(BF16) for h in range(heads)], axis=1
    )
    out_ref[...] = jnp.dot(attended, w_ref[...], preferred_element_type=F32)


def vmem(x):
    return pltpu.with_memory_space_constraint(x, pltpu.VMEM)


def in_vmem(count):
    return [pl.BlockSpec(memory_space=pltpu.VMEM)] * count


def exchange_steps(axis):
    size = lax.axis_size(axis)
    assert size & (size - 1) == 0
    steps, low = [], 1
    while low < size:
        steps.append([low, 2 * low, 3 * low] if 4 * low <= size else [low])
        low *= len(steps[-1]) + 1
    return steps


def gather_from(value, axis, distances):
    size = lax.axis_size(axis)
    return [value] + [lax.ppermute(value, axis, [(i, i ^ d) for i in range(size)]) for d in distances]


def rope_tables(span, kv, width):
    half = width // 2
    index = np.arange(half, dtype=np.float32)
    freq = np.exp(index * np.float32(-2.0 * math.log(THETA_BASE) / width)).astype(np.float32)
    angle = np.arange(span, dtype=np.float32)[:, None] * freq
    cos_part, sin_part = np.cos(angle.astype(np.float64)), np.sin(angle.astype(np.float64))
    both = np.stack([np.concatenate([cos_part, cos_part], 1), np.concatenate([-sin_part, sin_part], 1)])
    return np.repeat(both, kv, axis=1).astype(np.float32)


def body(query, key_cache, value_cache, new_key, new_value, lengths, out_weight):
    seq_count = lax.axis_size("seq")
    batch, span, kv, width = key_cache.shape
    heads = query.shape[1]
    stretch = span * seq_count // 8
    rows = span * kv
    chunks = 4
    lanes = batch * SLOT
    packed_rows = heads * batch + batch
    if span == stretch:
        tables = jnp.asarray(rope_tables(span, kv, width))
    else:
        tables = jnp.zeros((2, 8, width), F32)
    dma = pltpu.SemaphoreType.DMA
    packed, weight = pl.pallas_call(
        functools.partial(attention_kernel, stretch=stretch, kv=kv, chunks=chunks),
        out_shape=[pltpu.VMEM((packed_rows, width), F32), pltpu.VMEM(out_weight.shape, BF16)],
        in_specs=[pl.BlockSpec(memory_space=pl.ANY)] * 8,
        out_specs=in_vmem(2),
        scratch_shapes=[
            pltpu.VMEM((2, rows, width), F32),
            pltpu.SMEM((batch,), jnp.int32),
            pltpu.VMEM((heads, batch, width), BF16),
            pltpu.VMEM((batch, kv, width), BF16),
            pltpu.VMEM((batch, kv, width), BF16),
            pltpu.VMEM((batch, rows, width), BF16),
            pltpu.VMEM((batch, rows, width), BF16),
            pltpu.VMEM((batch, rows // chunks, width), BF16),
            pltpu.VMEM((batch, rows // chunks, width), BF16),
            pltpu.VMEM((lanes, batch * width), BF16),
            pltpu.VMEM((lanes, width), BF16),
            pltpu.VMEM((2, heads * batch, width), F32),
            pltpu.VMEM((rows, lanes), F32),
            dma((chunks,)), dma((chunks,)), dma((batch // 2,)), dma, dma, dma, dma, dma,
        ],
        name="attention",
    )(
        tables, lengths, jnp.transpose(query, (1, 0, 2)), new_key, new_value,
        key_cache.reshape(batch, rows, width), value_cache.reshape(batch, rows, width),
        out_weight,
    )
    steps = exchange_steps("seq")
    for distances in steps[:-1]:
        parts = gather_from(packed, "seq", distances)
        packed = pl.pallas_call(
            functools.partial(merge_kernel, heads=heads, batch=batch),
            out_shape=pltpu.VMEM(packed.shape, F32),
            in_specs=in_vmem(len(parts)),
            out_specs=in_vmem(1)[0],
            name="merge",
        )(*map(vmem, parts))
    parts = gather_from(packed, "seq", steps[-1])
    share = pl.pallas_call(
        functools.partial(project_kernel, heads=heads, batch=batch),
        out_shape=pltpu.VMEM((batch, out_weight.shape[1]), F32),
        in_specs=in_vmem(len(parts) + 1),
        out_specs=in_vmem(1)[0],
        name="project",
    )(*map(vmem, parts), vmem(weight))
    for distances in exchange_steps("head"):
        share = balanced_sum(gather_from(share, "head", distances))
    return share


def solution(mesh):
    placed = (
        P(None, "head", None),
        P(None, "seq", "head", None),
        P(None, "seq", "head", None),
        P(None, "head", None),
        P(None, "head", None),
        P(),
        P("head", "seq"),
    )
    return jax.shard_map(
        body, mesh=mesh, in_specs=placed, out_specs=P(None, "seq"), check_vma=False
    )
```

```python
import functools
import math

import jax
import jax.numpy as jnp
from jax import lax
from jax.experimental import pallas as pl
from jax.experimental.pallas import tpu as pltpu
from jax.sharding import PartitionSpec as P
import numpy as np

THETA_BASE = 10000000.0
NEG_FILL = -1e30
SLOT = 16
F32 = jnp.float32
BF16 = jnp.bfloat16


def frequencies(shape):
    width = shape[-1]
    half = width // 2
    lane = lax.broadcasted_iota(jnp.int32, shape, len(shape) - 1)
    index = jnp.where(lane < half, lane, lane - half).astype(F32)
    return jnp.exp(index * F32(-2.0 * math.log(THETA_BASE) / width))


def half_sign(shape):
    lane = lax.broadcasted_iota(jnp.int32, shape, len(shape) - 1)
    return jnp.where(lane < shape[-1] // 2, F32(-1.0), F32(1.0))


def rotate(values, cos_part, signed_sin):
    return values * cos_part + pltpu.roll(values, values.shape[-1] // 2, 1) * signed_sin


def rows_of_scalars(scalars, shape):
    row = lax.broadcasted_iota(jnp.int32, shape, 0)
    out = jnp.zeros(shape, scalars[0].dtype)
    for i, s in enumerate(scalars):
        out = jnp.where(row == i, s, out)
    return out


def attention_kernel(
    tab_hbm, lens_hbm, q_hbm, nk_hbm, nv_hbm, k_hbm, v_hbm, w_hbm,
    out_ref, w_ref,
    tab_raw, tab, lens, qbuf, nkbuf, nvbuf, kbuf, vbuf, kcat0, kcat1, qbd, qin, qrot, scores,
    tsem, ksem, vsem, lsem, qsem, nksem, nvsem, wsem, order,
    *, stretch, kv, chunks,
):
    batch, rows, width = kbuf.shape
    heads = qbuf.shape[0]
    group = heads // kv
    lanes = batch * SLOT
    span = rows // kv
    chunk = rows // chunks
    pairs = batch // 2
    whole_stretch = span == stretch
    kcats = (kcat0, kcat1)

    def kcopy(c):
        part = pl.ds(c * chunk, chunk)
        return pltpu.make_async_copy(k_hbm.at[:, part, :], kbuf.at[:, part, :], ksem.at[c])

    vcopy = pltpu.make_async_copy(v_hbm, vbuf, vsem)
    tcopy = pltpu.make_async_copy(tab_hbm, tab_raw, tsem)
    wcopy = pltpu.make_async_copy(w_hbm, w_ref, wsem)

    lcopy = pltpu.make_async_copy(lens_hbm, lens, lsem)
    qcopy = pltpu.make_async_copy(q_hbm, qbuf, qsem)
    nkcopy = pltpu.make_async_copy(nk_hbm, nkbuf, nksem)
    nvcopy = pltpu.make_async_copy(nv_hbm, nvbuf, nvsem)
    small = (lcopy, qcopy, nkcopy, nvcopy)
    for copy in small:
        copy.start()
    if whole_stretch:
        tcopy.start()
    pl.semaphore_signal(order, 1)
    pl.semaphore_wait(order, 1)
    for c in range(chunks):
        kcopy(c).start()
    vcopy.start()

    place = lax.axis_index("seq").astype(jnp.int32)
    base = place * span
    key_stretch = base // stretch

    qbd[...] = jnp.zeros_like(qbd)
    qin[...] = jnp.zeros_like(qin)
    freq8 = frequencies((batch, width))
    sign8 = half_sign((batch, width))
    if not whole_stretch:
        row = lax.broadcasted_iota(jnp.int32, (rows, width), 0)
        angle = (base % stretch + row // kv).astype(F32) * frequencies((rows, width))
        tab[0] = jnp.cos(angle)
        tab[1] = jnp.sin(angle) * half_sign((rows, width))

    for copy in small:
        copy.wait()
    if whole_stretch:
        tcopy.wait()
        lower = lax.broadcasted_iota(jnp.int32, (8, width), 1) < width // 2
        for i in range(span // 8):
            t = tab_raw[8 * i : 8 * i + 8, :]
            other = pltpu.roll(t, width // 2, 1)
            cos_part, sin_part = jnp.where(lower, t, other), jnp.where(lower, -other, t)
            for j in range(kv):
                at = pl.ds(8 * kv * i + j, 8, stride=kv)
                tab[0, at, :] = cos_part
                tab[1, at, :] = sin_part
    picked, intra, limit = [], [], []
    for b in range(batch):
        p = lens[b]
        qc = p // stretch
        r = p - qc * stretch
        intra.append(r.astype(F32))
        inter = stretch + stretch // 2
        picked.append(
            jnp.where(key_stretch == qc, r, jnp.where(key_stretch == qc - 1, r + stretch, inter)).astype(F32)
        )
        limit.append((p - base) * kv)
    angle_p = rows_of_scalars(picked, (batch, width)) * freq8
    angle_r = rows_of_scalars(intra, (batch, width)) * freq8
    cp, sp = jnp.cos(angle_p), jnp.sin(angle_p) * sign8
    cr, sr = jnp.cos(angle_r), jnp.sin(angle_r) * sign8

    for h in range(heads):
        q = qbuf[h].astype(F32)
        at = slice(h * batch, (h + 1) * batch)
        qrot[0, at, :] = rotate(q, cp, sp)
        qrot[1, at, :] = rotate(q, cr, sr)
    for b in range(batch):
        mine = pl.ds(b, heads, stride=batch)
        at = slice(b * SLOT, b * SLOT + heads)
        qbd[at, b * width : (b + 1) * width] = qrot[0, mine, :].astype(BF16)
        qin[at, :] = qrot[1, mine, :].astype(BF16)

    scaling = F32(1.0 / math.sqrt(width))

    lane1 = lax.broadcasted_iota(jnp.int32, (1, lanes), 1)
    bound = jnp.zeros((1, lanes), jnp.int32)
    for b in range(batch):
        bound = jnp.where(lane1 // SLOT == b, limit[b], bound)
    lane_kv = jnp.minimum((lane1 % SLOT) // group, kv - 1)
    row_c = lax.broadcasted_iota(jnp.int32, (chunk, lanes), 0)
    fits = row_c % kv == lane_kv

    def rotate_keys(c):
        part = slice(c * chunk, (c + 1) * chunk)
        for b in range(batch):
            k = kbuf[b, part, :]
            turned = pltpu.roll(k, width // 2, 1).astype(F32)
            k = k.astype(F32) * tab[0, part, :] + turned * tab[1, part, :]
            kcats[c % 2][b] = k.astype(BF16)

    def score(c, top):
        sums = []
        for g in range(2):
            keys = jnp.concatenate([kcats[c % 2][b, g*chunk//2:(g+1)*chunk//2] for b in range(batch)], axis=1)
            sums.append(lax.dot_general(
                keys, qbd[...],
                (((1,), (1,)), ((), ())), preferred_element_type=F32,
            ))
        s = jnp.concatenate(sums, axis=0) * scaling
        s = jnp.where(fits & (row_c + c * chunk < bound), s, F32(NEG_FILL))
        scores[c * chunk : (c + 1) * chunk, :] = s
        return jnp.maximum(top, jnp.max(s, axis=0, keepdims=True))

    for c in range(chunks):
        kcopy(c).wait()
        if c == chunks - 1:
            wcopy.start()
        rotate_keys(c)
        if c == 1:
            own_rows = batch * kv
            knew = jnp.concatenate(
                [rotate(nkbuf[b].astype(F32), cr[b : b + 1], sr[b : b + 1]) for b in range(batch)], axis=0
            ).astype(BF16)
            own_all = lax.dot_general(
                knew, qin[...], (((1,), (1,)), ((), ())), preferred_element_type=F32
            ) * scaling
            own_row = lax.broadcasted_iota(jnp.int32, (own_rows, lanes), 0)
            own_lane = lax.broadcasted_iota(jnp.int32, (own_rows, lanes), 1)
            own_kv = jnp.minimum((own_lane % SLOT) // group, kv - 1)
            own_mask = (own_row // kv == own_lane // SLOT) & (own_row % kv == own_kv)
            own = jnp.sum(jnp.where(own_mask, own_all, 0.0), axis=0, keepdims=True)
            first = place == 0
            own = jnp.where(first, own, F32(NEG_FILL))
            top = own
        if c:
            top = score(c - 1, top)
    vcopy.wait()
    top = score(chunks - 1, top)

    own_w = jnp.where(first, jnp.exp(own - top), 0.0)
    total = own_w
    parts = []
    for c in range(chunks):
        s = scores[c * chunk : (c + 1) * chunk, :]
        w = jnp.where(s > F32(0.5 * NEG_FILL), jnp.exp(s - top), 0.0)
        total = total + jnp.sum(w, axis=0, keepdims=True)
        parts.append(jnp.transpose(w.astype(BF16)))
    wt = jnp.concatenate(parts, axis=1)

    own_wt = jnp.transpose(jnp.where(own_mask, own_w, 0.0))
    nv = jnp.concatenate([nvbuf[b].astype(F32) for b in range(batch)], axis=0)
    own_acc = lax.dot_general(
        own_wt, nv, (((1,), (0,)), ((), ())), preferred_element_type=F32,
        precision=lax.Precision.HIGHEST,
    )

    for c in range(pairs):
        v = jnp.concatenate([vbuf[2 * c], vbuf[2 * c + 1]], axis=1)
        acc = jnp.dot(wt[2 * c * SLOT : (2 * c + 2) * SLOT, :], v, preferred_element_type=F32)
        for j in range(2):
            b = 2 * c + j
            part = acc[j * SLOT : (j + 1) * SLOT, j * width : (j + 1) * width]
            part = part + own_acc[b * SLOT : (b + 1) * SLOT, :]
            out_ref[pl.ds(b, heads, stride=batch), :] = part[:heads]

    lane_b = lax.broadcasted_iota(jnp.int32, (batch, lanes), 1)
    row_b = lax.broadcasted_iota(jnp.int32, (batch, lanes), 0)
    stats = jnp.zeros((batch, lanes), F32)
    for b in range(batch):
        m_b = pltpu.roll(top, (lanes - b * SLOT) % lanes, 1) if b else top
        l_b = pltpu.roll(total, (lanes + SLOT - b * SLOT) % lanes, 1) if b != 1 else total
        stats = jnp.where(row_b == b, jnp.where(lane_b < SLOT, m_b, l_b), stats)
    out_ref[heads * batch :, :] = stats
    wcopy.wait()


def balanced_sum(values):
    while len(values) > 1:
        values = [values[i] + values[i + 1] for i in range(0, len(values), 2)]
    return values[0]


def merge(parts, heads, batch):
    stats = [p[heads * batch :, :] for p in parts]
    top = functools.reduce(jnp.maximum, stats)
    factors = [jnp.exp(s - top) for s in stats]
    total = balanced_sum([s * pltpu.roll(f, SLOT, 1) for s, f in zip(stats, factors)])
    lane = lax.broadcasted_iota(jnp.int32, top.shape, 1)
    sums = []
    for h in range(heads):
        rows = slice(h * batch, (h + 1) * batch)
        sums.append(balanced_sum([p[rows, :] * f[:, h : h + 1] for p, f in zip(parts, factors)]))
    return sums, jnp.where(lane < SLOT, top, total)


def merge_kernel(*refs, heads, batch):
    out_ref = refs[-1]
    sums, stats = merge(refs[:-1], heads, batch)
    for h in range(heads):
        out_ref[h * batch : (h + 1) * batch, :] = sums[h]
    out_ref[heads * batch :, :] = stats


def project_kernel(*refs, heads, batch):
    w_ref, out_ref = refs[-2:]
    sums, stats = merge(refs[:-2], heads, batch)
    attended = jnp.concatenate(
        [(sums[h] / stats[:, SLOT + h : SLOT + h + 1]).astype(BF16) for h in range(heads)], axis=1
    )
    out_ref[...] = jnp.dot(attended, w_ref[...], preferred_element_type=F32)


def vmem(x):
    return pltpu.with_memory_space_constraint(x, pltpu.VMEM)


def in_vmem(count):
    return [pl.BlockSpec(memory_space=pltpu.VMEM)] * count


def exchange_steps(axis):
    size = lax.axis_size(axis)
    assert size & (size - 1) == 0
    steps, low = [], 1
    while low < size:
        steps.append([low, 2 * low, 3 * low] if 4 * low <= size else [low])
        low *= len(steps[-1]) + 1
    return steps


def gather_from(value, axis, distances):
    size = lax.axis_size(axis)
    return [value] + [lax.ppermute(value, axis, [(i, i ^ d) for i in range(size)]) for d in distances]


def rope_table(span, width):
    half = width // 2
    index = np.arange(half, dtype=np.float32)
    freq = np.exp(index * np.float32(-2.0 * math.log(THETA_BASE) / width)).astype(np.float32)
    angle = (np.arange(span, dtype=np.float32)[:, None] * freq).astype(np.float64)
    return np.concatenate([np.cos(angle), np.sin(angle)], axis=1).astype(np.float32)


def body(query, key_cache, value_cache, new_key, new_value, lengths, out_weight):
    seq_count = lax.axis_size("seq")
    batch, span, kv, width = key_cache.shape
    heads = query.shape[1]
    stretch = span * seq_count // 8
    rows = span * kv
    chunks = 4
    lanes = batch * SLOT
    packed_rows = heads * batch + batch
    if span == stretch:
        tables = jnp.asarray(rope_table(span, width))
    else:
        tables = jnp.zeros((8, width), F32)
    dma = pltpu.SemaphoreType.DMA
    packed, weight = pl.pallas_call(
        functools.partial(attention_kernel, stretch=stretch, kv=kv, chunks=chunks),
        out_shape=[pltpu.VMEM((packed_rows, width), F32), pltpu.VMEM(out_weight.shape, BF16)],
        in_specs=[pl.BlockSpec(memory_space=pl.ANY)] * 8,
        out_specs=in_vmem(2),
        scratch_shapes=[
            pltpu.VMEM(tables.shape, F32),
            pltpu.VMEM((2, rows, width), F32),
            pltpu.SMEM((batch,), jnp.int32),
            pltpu.VMEM((heads, batch, width), BF16),
            pltpu.VMEM((batch, kv, width), BF16),
            pltpu.VMEM((batch, kv, width), BF16),
            pltpu.VMEM((batch, rows, width), BF16),
            pltpu.VMEM((batch, rows, width), BF16),
            pltpu.VMEM((batch, rows // chunks, width), BF16),
            pltpu.VMEM((batch, rows // chunks, width), BF16),
            pltpu.VMEM((lanes, batch * width), BF16),
            pltpu.VMEM((lanes, width), BF16),
            pltpu.VMEM((2, heads * batch, width), F32),
            pltpu.VMEM((rows, lanes), F32),
            dma, dma((chunks,)), dma, dma, dma, dma, dma, dma, pltpu.SemaphoreType.REGULAR,
        ],
        name="attention",
    )(
        tables, lengths, jnp.transpose(query, (1, 0, 2)), new_key, new_value,
        key_cache.reshape(batch, rows, width), value_cache.reshape(batch, rows, width),
        out_weight,
    )
    steps = exchange_steps("seq")
    for distances in steps[:-1]:
        parts = gather_from(packed, "seq", distances)
        packed = pl.pallas_call(
            functools.partial(merge_kernel, heads=heads, batch=batch),
            out_shape=pltpu.VMEM(packed.shape, F32),
            in_specs=in_vmem(len(parts)),
            out_specs=in_vmem(1)[0],
            name="merge",
        )(*map(vmem, parts))
    parts = gather_from(packed, "seq", steps[-1])
    share = pl.pallas_call(
        functools.partial(project_kernel, heads=heads, batch=batch),
        out_shape=pltpu.VMEM((batch, out_weight.shape[1]), F32),
        in_specs=in_vmem(len(parts) + 1),
        out_specs=in_vmem(1)[0],
        name="project",
    )(*map(vmem, parts), vmem(weight))
    for distances in exchange_steps("head"):
        share = balanced_sum(gather_from(share, "head", distances))
    return share


def solution(mesh):
    placed = (
        P(None, "head", None),
        P(None, "seq", "head", None),
        P(None, "seq", "head", None),
        P(None, "head", None),
        P(None, "head", None),
        P(),
        P("head", "seq"),
    )
    return jax.shard_map(
        body, mesh=mesh, in_specs=placed, out_specs=P(None, "seq"), check_vma=False
    )
```

```python
import functools
import math

import jax
import jax.numpy as jnp
from jax import lax
from jax.experimental import pallas as pl
from jax.experimental.pallas import tpu as pltpu
from jax.sharding import PartitionSpec as P

THETA_BASE = 10000000.0
NEG_FILL = -1e30
RUN = 32
SLOT = 16
F32 = jnp.float32
BF16 = jnp.bfloat16


def frequencies(shape):
    width = shape[-1]
    half = width // 2
    lane = lax.broadcasted_iota(jnp.int32, shape, len(shape) - 1)
    index = jnp.where(lane < half, lane, lane - half).astype(F32)
    return jnp.exp(index * F32(-2.0 * math.log(THETA_BASE) / width))


def half_sign(shape):
    lane = lax.broadcasted_iota(jnp.int32, shape, len(shape) - 1)
    return jnp.where(lane < shape[-1] // 2, F32(-1.0), F32(1.0))


def rotate(values, cos_part, signed_sin):
    return values * cos_part + pltpu.roll(values, values.shape[-1] // 2, 1) * signed_sin


def rows_of_scalars(scalars, shape):
    row = lax.broadcasted_iota(jnp.int32, shape, 0)
    out = jnp.zeros(shape, scalars[0].dtype)
    for i, s in enumerate(scalars):
        out = jnp.where(row == i, s, out)
    return out


def attention_kernel(
    lens_hbm, q_hbm, nk_hbm, nv_hbm, k_hbm, v_hbm, w_hbm,
    out_ref, w_ref,
    tab, lens, qbuf, nkbuf, nvbuf, kbuf, vbuf, kcat0, kcat1, qbd, qin, qrot, scores,
    ksem, vsem, lsem, qsem, nksem, nvsem, wsem, order,
    *, stretch, kv, sizes,
):
    batch, rows, width = kbuf.shape
    heads = qbuf.shape[0]
    group = heads // kv
    lanes = batch * SLOT
    span = rows // kv
    chunks = len(sizes)
    parts_at = [slice(sum(sizes[:c]), sum(sizes[: c + 1])) for c in range(chunks)]
    pairs = batch // 2
    kcats = (kcat0, kcat1)

    def kcopy(c):
        part = pl.ds(parts_at[c].start, sizes[c])
        return pltpu.make_async_copy(k_hbm.at[:, part, :], kbuf.at[:, part, :], ksem.at[c])

    vcopy = pltpu.make_async_copy(v_hbm, vbuf, vsem)
    wcopy = pltpu.make_async_copy(w_hbm, w_ref, wsem)

    lcopy = pltpu.make_async_copy(lens_hbm, lens, lsem)
    qcopy = pltpu.make_async_copy(q_hbm, qbuf, qsem)
    nkcopy = pltpu.make_async_copy(nk_hbm, nkbuf, nksem)
    nvcopy = pltpu.make_async_copy(nv_hbm, nvbuf, nvsem)
    small = (lcopy, qcopy, nkcopy, nvcopy)
    for copy in small:
        copy.start()
    pl.semaphore_signal(order, 1)
    pl.semaphore_wait(order, 1)
    for c in range(chunks):
        kcopy(c).start()
    vcopy.start()

    place = lax.axis_index("seq").astype(jnp.int32)
    base = place * span
    key_stretch = base // stretch

    qbd[...] = jnp.zeros_like(qbd)
    qin[...] = jnp.zeros_like(qin)
    freq8 = frequencies((batch, width))
    sign8 = half_sign((batch, width))

    runs = span // RUN
    start = (base % stretch).astype(F32)
    far = start + (RUN * lax.broadcasted_iota(jnp.int32, (runs, width), 0)).astype(F32)
    far = far * frequencies((runs, width))
    far_c, far_s = jnp.cos(far), jnp.sin(far) * half_sign((runs, width))
    near = lax.broadcasted_iota(jnp.int32, (RUN, width), 0).astype(F32) * frequencies((RUN, width))
    near_c, near_signed = jnp.cos(near), jnp.sin(near) * half_sign((RUN, width))
    for i in range(runs):
        c_i, s_i = far_c[i : i + 1], far_s[i : i + 1]
        cos_part = c_i * near_c - s_i * near_signed
        sin_part = s_i * near_c + c_i * near_signed
        for j in range(kv):
            at = pl.ds(RUN * kv * i + j, RUN, stride=kv)
            tab[0, at, :] = cos_part
            tab[1, at, :] = sin_part

    for copy in small:
        copy.wait()
    picked, intra, limit = [], [], []
    for b in range(batch):
        p = lens[b]
        qc = p // stretch
        r = p - qc * stretch
        intra.append(r.astype(F32))
        inter = stretch + stretch // 2
        picked.append(
            jnp.where(key_stretch == qc, r, jnp.where(key_stretch == qc - 1, r + stretch, inter)).astype(F32)
        )
        limit.append((p - base) * kv)
    angle_p = rows_of_scalars(picked, (batch, width)) * freq8
    angle_r = rows_of_scalars(intra, (batch, width)) * freq8
    cp, sp = jnp.cos(angle_p), jnp.sin(angle_p) * sign8
    cr, sr = jnp.cos(angle_r), jnp.sin(angle_r) * sign8

    for h in range(heads):
        q = qbuf[h].astype(F32)
        at = slice(h * batch, (h + 1) * batch)
        qrot[0, at, :] = rotate(q, cp, sp)
        qrot[1, at, :] = rotate(q, cr, sr)
    for b in range(batch):
        mine = pl.ds(b, heads, stride=batch)
        at = slice(b * SLOT, b * SLOT + heads)
        qbd[at, b * width : (b + 1) * width] = qrot[0, mine, :].astype(BF16)
        qin[at, :] = qrot[1, mine, :].astype(BF16)

    scaling = F32(1.0 / math.sqrt(width))

    lane1 = lax.broadcasted_iota(jnp.int32, (1, lanes), 1)
    bound = jnp.zeros((1, lanes), jnp.int32)
    for b in range(batch):
        bound = jnp.where(lane1 // SLOT == b, limit[b], bound)
    lane_kv = jnp.minimum((lane1 % SLOT) // group, kv - 1)

    def rotate_keys(c):
        part = parts_at[c]
        for b in range(batch):
            k = kbuf[b, part, :]
            turned = pltpu.roll(k, width // 2, 1).astype(F32)
            k = k.astype(F32) * tab[0, part, :] + turned * tab[1, part, :]
            kcats[c % 2][b, : sizes[c], :] = k.astype(BF16)

    def score(c, top):
        half = sizes[c] // 2
        sums = []
        for part in (slice(0, half), slice(half, sizes[c])):
            keys = jnp.concatenate([kcats[c % 2][b, part, :] for b in range(batch)], axis=1)
            sums.append(lax.dot_general(
                keys, qbd[...], (((1,), (1,)), ((), ())), preferred_element_type=F32
            ))
        s = jnp.concatenate(sums, axis=0) * scaling
        row = parts_at[c].start + lax.broadcasted_iota(jnp.int32, s.shape, 0)
        s = jnp.where((row % kv == lane_kv) & (row < bound), s, F32(NEG_FILL))
        scores[parts_at[c], :] = s
        return jnp.maximum(top, jnp.max(s, axis=0, keepdims=True))

    for c in range(chunks):
        kcopy(c).wait()
        if c == chunks - 1:
            wcopy.start()
        rotate_keys(c)
        if c == 1:
            own_rows = batch * kv
            knew = jnp.concatenate(
                [rotate(nkbuf[b].astype(F32), cr[b : b + 1], sr[b : b + 1]) for b in range(batch)], axis=0
            ).astype(BF16)
            own_all = lax.dot_general(
                knew, qin[...], (((1,), (1,)), ((), ())), preferred_element_type=F32
            ) * scaling
            own_row = lax.broadcasted_iota(jnp.int32, (own_rows, lanes), 0)
            own_lane = lax.broadcasted_iota(jnp.int32, (own_rows, lanes), 1)
            own_kv = jnp.minimum((own_lane % SLOT) // group, kv - 1)
            own_mask = (own_row // kv == own_lane // SLOT) & (own_row % kv == own_kv)
            own = jnp.sum(jnp.where(own_mask, own_all, 0.0), axis=0, keepdims=True)
            first = place == 0
            own = jnp.where(first, own, F32(NEG_FILL))
            top = own
        if c:
            top = score(c - 1, top)
    vcopy.wait()
    top = score(chunks - 1, top)

    own_w = jnp.where(first, jnp.exp(own - top), 0.0)
    total = own_w
    parts = []
    for c in range(chunks):
        s = scores[parts_at[c], :]
        w = jnp.where(s > F32(0.5 * NEG_FILL), jnp.exp(s - top), 0.0)
        total = total + jnp.sum(w, axis=0, keepdims=True)
        parts.append(jnp.transpose(w.astype(BF16)))
    wt = jnp.concatenate(parts, axis=1)

    own_wt = jnp.transpose(jnp.where(own_mask, own_w, 0.0))
    nv = jnp.concatenate([nvbuf[b].astype(F32) for b in range(batch)], axis=0)
    own_acc = lax.dot_general(
        own_wt, nv, (((1,), (0,)), ((), ())), preferred_element_type=F32,
        precision=lax.Precision.HIGHEST,
    )

    for c in range(pairs):
        v = jnp.concatenate([vbuf[2 * c], vbuf[2 * c + 1]], axis=1)
        acc = jnp.dot(wt[2 * c * SLOT : (2 * c + 2) * SLOT, :], v, preferred_element_type=F32)
        for j in range(2):
            b = 2 * c + j
            part = acc[j * SLOT : (j + 1) * SLOT, j * width : (j + 1) * width]
            part = part + own_acc[b * SLOT : (b + 1) * SLOT, :]
            out_ref[pl.ds(b, heads, stride=batch), :] = part[:heads]

    lane_b = lax.broadcasted_iota(jnp.int32, (batch, lanes), 1)
    row_b = lax.broadcasted_iota(jnp.int32, (batch, lanes), 0)
    stats = jnp.zeros((batch, lanes), F32)
    for b in range(batch):
        m_b = pltpu.roll(top, (lanes - b * SLOT) % lanes, 1) if b else top
        l_b = pltpu.roll(total, (lanes + SLOT - b * SLOT) % lanes, 1) if b != 1 else total
        stats = jnp.where(row_b == b, jnp.where(lane_b < SLOT, m_b, l_b), stats)
    out_ref[heads * batch :, :] = stats
    wcopy.wait()


def balanced_sum(values):
    while len(values) > 1:
        values = [values[i] + values[i + 1] for i in range(0, len(values), 2)]
    return values[0]


def merge(parts, heads, batch):
    stats = [p[heads * batch :, :] for p in parts]
    top = functools.reduce(jnp.maximum, stats)
    factors = [jnp.exp(s - top) for s in stats]
    total = balanced_sum([s * pltpu.roll(f, SLOT, 1) for s, f in zip(stats, factors)])
    lane = lax.broadcasted_iota(jnp.int32, top.shape, 1)
    sums = []
    for h in range(heads):
        rows = slice(h * batch, (h + 1) * batch)
        sums.append(balanced_sum([p[rows, :] * f[:, h : h + 1] for p, f in zip(parts, factors)]))
    return sums, jnp.where(lane < SLOT, top, total)


def merge_kernel(*refs, heads, batch):
    out_ref = refs[-1]
    sums, stats = merge(refs[:-1], heads, batch)
    for h in range(heads):
        out_ref[h * batch : (h + 1) * batch, :] = sums[h]
    out_ref[heads * batch :, :] = stats


def project_kernel(*refs, heads, batch):
    w_ref, out_ref = refs[-2:]
    sums, stats = merge(refs[:-2], heads, batch)
    attended = jnp.concatenate(
        [(sums[h] / stats[:, SLOT + h : SLOT + h + 1]).astype(BF16) for h in range(heads)], axis=1
    )
    out_ref[...] = jnp.dot(attended, w_ref[...], preferred_element_type=F32)


def vmem(x):
    return pltpu.with_memory_space_constraint(x, pltpu.VMEM)


def in_vmem(count):
    return [pl.BlockSpec(memory_space=pltpu.VMEM)] * count


def exchange_steps(axis):
    size = lax.axis_size(axis)
    assert size & (size - 1) == 0
    steps, low = [], 1
    while low < size:
        steps.append([low, 2 * low, 3 * low] if 4 * low <= size else [low])
        low *= len(steps[-1]) + 1
    return steps


def gather_from(value, axis, distances):
    size = lax.axis_size(axis)
    return [value] + [lax.ppermute(value, axis, [(i, i ^ d) for i in range(size)]) for d in distances]


def body(query, key_cache, value_cache, new_key, new_value, lengths, out_weight):
    seq_count = lax.axis_size("seq")
    batch, span, kv, width = key_cache.shape
    heads = query.shape[1]
    stretch = span * seq_count // 8
    rows = span * kv
    sizes = [rows * n // 16 for n in (4, 5, 7)]
    lanes = batch * SLOT
    packed_rows = heads * batch + batch
    dma = pltpu.SemaphoreType.DMA
    packed, weight = pl.pallas_call(
        functools.partial(attention_kernel, stretch=stretch, kv=kv, sizes=sizes),
        out_shape=[pltpu.VMEM((packed_rows, width), F32), pltpu.VMEM(out_weight.shape, BF16)],
        in_specs=[pl.BlockSpec(memory_space=pl.ANY)] * 7,
        out_specs=in_vmem(2),
        scratch_shapes=[
            pltpu.VMEM((2, rows, width), F32),
            pltpu.SMEM((batch,), jnp.int32),
            pltpu.VMEM((heads, batch, width), BF16),
            pltpu.VMEM((batch, kv, width), BF16),
            pltpu.VMEM((batch, kv, width), BF16),
            pltpu.VMEM((batch, rows, width), BF16),
            pltpu.VMEM((batch, rows, width), BF16),
            pltpu.VMEM((batch, max(sizes), width), BF16),
            pltpu.VMEM((batch, max(sizes), width), BF16),
            pltpu.VMEM((lanes, batch * width), BF16),
            pltpu.VMEM((lanes, width), BF16),
            pltpu.VMEM((2, heads * batch, width), F32),
            pltpu.VMEM((rows, lanes), F32),
            dma((len(sizes),)), dma, dma, dma, dma, dma, dma, pltpu.SemaphoreType.REGULAR,
        ],
        name="attention",
    )(
        lengths, jnp.transpose(query, (1, 0, 2)), new_key, new_value,
        key_cache.reshape(batch, rows, width), value_cache.reshape(batch, rows, width),
        out_weight,
    )
    steps = exchange_steps("seq")
    for distances in steps[:-1]:
        parts = gather_from(packed, "seq", distances)
        packed = pl.pallas_call(
            functools.partial(merge_kernel, heads=heads, batch=batch),
            out_shape=pltpu.VMEM(packed.shape, F32),
            in_specs=in_vmem(len(parts)),
            out_specs=in_vmem(1)[0],
            name="merge",
        )(*map(vmem, parts))
    parts = gather_from(packed, "seq", steps[-1])
    share = pl.pallas_call(
        functools.partial(project_kernel, heads=heads, batch=batch),
        out_shape=pltpu.VMEM((batch, out_weight.shape[1]), F32),
        in_specs=in_vmem(len(parts) + 1),
        out_specs=in_vmem(1)[0],
        name="project",
    )(*map(vmem, parts), vmem(weight))
    for distances in exchange_steps("head"):
        share = balanced_sum(gather_from(share, "head", distances))
    return share


def solution(mesh):
    placed = (
        P(None, "head", None),
        P(None, "seq", "head", None),
        P(None, "seq", "head", None),
        P(None, "head", None),
        P(None, "head", None),
        P(),
        P("head", "seq"),
    )
    return jax.shard_map(
        body, mesh=mesh, in_specs=placed, out_specs=P(None, "seq"), check_vma=False
    )
```

```python
import functools
import math

import jax
import jax.numpy as jnp
from jax import lax
from jax.experimental import pallas as pl
from jax.experimental.pallas import tpu as pltpu
from jax.sharding import PartitionSpec as P

THETA_BASE = 10000000.0
NEG_FILL = -1e30
RUN = 32
SLOT = 16
F32 = jnp.float32
BF16 = jnp.bfloat16


def frequencies(shape):
    width = shape[-1]
    half = width // 2
    lane = lax.broadcasted_iota(jnp.int32, shape, len(shape) - 1)
    index = jnp.where(lane < half, lane, lane - half).astype(F32)
    return jnp.exp(index * F32(-2.0 * math.log(THETA_BASE) / width))


def half_sign(shape):
    lane = lax.broadcasted_iota(jnp.int32, shape, len(shape) - 1)
    return jnp.where(lane < shape[-1] // 2, F32(-1.0), F32(1.0))


def rotate(values, cos_part, signed_sin):
    return values * cos_part + pltpu.roll(values, values.shape[-1] // 2, 1) * signed_sin


def rows_of_scalars(scalars, shape):
    row = lax.broadcasted_iota(jnp.int32, shape, 0)
    out = jnp.zeros(shape, scalars[0].dtype)
    for i, s in enumerate(scalars):
        out = jnp.where(row == i, s, out)
    return out


def attention_kernel(
    lens_hbm, q_hbm, nk_hbm, nv_hbm, k_hbm, v_hbm, w_hbm,
    out_ref, w_ref,
    tab, lens, qbuf, nkbuf, nvbuf, kbuf, vbuf, kcat0, kcat1, qbd, qin, qrot, scores,
    ksem, vsem, lsem, qsem, nksem, nvsem, wsem, order,
    *, stretch, kv, sizes,
):
    batch, rows, width = kbuf.shape
    heads = qbuf.shape[0]
    group = heads // kv
    lanes = batch * SLOT
    span = rows // kv
    chunks = len(sizes)
    parts_at = [slice(sum(sizes[:c]), sum(sizes[: c + 1])) for c in range(chunks)]
    pairs = batch // 2
    kcats = (kcat0, kcat1)

    def kcopy(c):
        part = pl.ds(parts_at[c].start, sizes[c])
        return pltpu.make_async_copy(k_hbm.at[:, part, :], kbuf.at[:, part, :], ksem.at[c])

    vcopy = pltpu.make_async_copy(v_hbm, vbuf, vsem)
    wcopy = pltpu.make_async_copy(w_hbm, w_ref, wsem)

    lcopy = pltpu.make_async_copy(lens_hbm, lens, lsem)
    qcopy = pltpu.make_async_copy(q_hbm, qbuf, qsem)
    nkcopy = pltpu.make_async_copy(nk_hbm, nkbuf, nksem)
    nvcopy = pltpu.make_async_copy(nv_hbm, nvbuf, nvsem)
    small = (lcopy, qcopy, nkcopy, nvcopy)
    for copy in small:
        copy.start()
    pl.semaphore_signal(order, 1)
    pl.semaphore_wait(order, 1)
    for c in range(chunks):
        kcopy(c).start()
    vcopy.start()

    place = lax.axis_index("seq").astype(jnp.int32)
    base = place * span
    key_stretch = base // stretch

    qbd[...] = jnp.zeros_like(qbd)
    qin[...] = jnp.zeros_like(qin)
    freq8 = frequencies((batch, width))
    sign8 = half_sign((batch, width))

    runs = span // RUN
    start = (base % stretch).astype(F32)
    far = start + (RUN * lax.broadcasted_iota(jnp.int32, (runs, width), 0)).astype(F32)
    far = far * frequencies((runs, width))
    far_c, far_s = jnp.cos(far), jnp.sin(far) * half_sign((runs, width))
    near = lax.broadcasted_iota(jnp.int32, (RUN, width), 0).astype(F32) * frequencies((RUN, width))
    near_c, near_signed = jnp.cos(near), jnp.sin(near) * half_sign((RUN, width))
    for i in range(runs):
        c_i, s_i = far_c[i : i + 1], far_s[i : i + 1]
        cos_part = c_i * near_c - s_i * near_signed
        sin_part = s_i * near_c + c_i * near_signed
        for j in range(kv):
            at = pl.ds(RUN * kv * i + j, RUN, stride=kv)
            tab[0, at, :] = cos_part
            tab[1, at, :] = sin_part

    for copy in small:
        copy.wait()
    picked, intra, limit = [], [], []
    for b in range(batch):
        p = lens[b]
        qc = p // stretch
        r = p - qc * stretch
        intra.append(r.astype(F32))
        inter = stretch + stretch // 2
        picked.append(
            jnp.where(key_stretch == qc, r, jnp.where(key_stretch == qc - 1, r + stretch, inter)).astype(F32)
        )
        limit.append((p - base) * kv)
    angle_p = rows_of_scalars(picked, (batch, width)) * freq8
    angle_r = rows_of_scalars(intra, (batch, width)) * freq8
    cp, sp = jnp.cos(angle_p), jnp.sin(angle_p) * sign8
    cr, sr = jnp.cos(angle_r), jnp.sin(angle_r) * sign8

    for h in range(heads):
        q = qbuf[h].astype(F32)
        at = slice(h * batch, (h + 1) * batch)
        qrot[0, at, :] = rotate(q, cp, sp)
        qrot[1, at, :] = rotate(q, cr, sr)
    for b in range(batch):
        mine = pl.ds(b, heads, stride=batch)
        at = slice(b * SLOT, b * SLOT + heads)
        qbd[at, b * width : (b + 1) * width] = qrot[0, mine, :].astype(BF16)
        qin[at, :] = qrot[1, mine, :].astype(BF16)

    scaling = F32(1.0 / math.sqrt(width))

    lane1 = lax.broadcasted_iota(jnp.int32, (1, lanes), 1)
    bound = jnp.zeros((1, lanes), jnp.int32)
    for b in range(batch):
        bound = jnp.where(lane1 // SLOT == b, limit[b], bound)
    lane_kv = jnp.minimum((lane1 % SLOT) // group, kv - 1)

    def rotate_keys(c):
        part = parts_at[c]
        for b in range(batch):
            k = kbuf[b, part, :]
            turned = pltpu.roll(k, width // 2, 1).astype(F32)
            k = k.astype(F32) * tab[0, part, :] + turned * tab[1, part, :]
            kcats[c % 2][b, : sizes[c], :] = k.astype(BF16)

    def score(c, top):
        half = sizes[c] // 2
        sums = []
        for part in (slice(0, half), slice(half, sizes[c])):
            keys = jnp.concatenate([kcats[c % 2][b, part, :] for b in range(batch)], axis=1)
            sums.append(lax.dot_general(
                keys, qbd[...], (((1,), (1,)), ((), ())), preferred_element_type=F32
            ))
        s = jnp.concatenate(sums, axis=0) * scaling
        row = parts_at[c].start + lax.broadcasted_iota(jnp.int32, s.shape, 0)
        s = jnp.where((row % kv == lane_kv) & (row < bound), s, F32(NEG_FILL))
        scores[parts_at[c], :] = s
        return jnp.maximum(top, jnp.max(s, axis=0, keepdims=True))

    for c in range(chunks):
        kcopy(c).wait()
        if c == chunks - 1:
            wcopy.start()
        rotate_keys(c)
        if c == 1:
            own_rows = batch * kv
            knew = jnp.concatenate(
                [rotate(nkbuf[b].astype(F32), cr[b : b + 1], sr[b : b + 1]) for b in range(batch)], axis=0
            ).astype(BF16)
            own_all = lax.dot_general(
                knew, qin[...], (((1,), (1,)), ((), ())), preferred_element_type=F32
            ) * scaling
            own_row = lax.broadcasted_iota(jnp.int32, (own_rows, lanes), 0)
            own_lane = lax.broadcasted_iota(jnp.int32, (own_rows, lanes), 1)
            own_kv = jnp.minimum((own_lane % SLOT) // group, kv - 1)
            own_mask = (own_row // kv == own_lane // SLOT) & (own_row % kv == own_kv)
            own = jnp.sum(jnp.where(own_mask, own_all, 0.0), axis=0, keepdims=True)
            first = place == 0
            own = jnp.where(first, own, F32(NEG_FILL))
            top = own
        if c:
            top = score(c - 1, top)
    vcopy.wait()
    top = score(chunks - 1, top)

    own_w = jnp.where(first, jnp.exp(own - top), 0.0)
    total = own_w
    parts = []
    for c in range(chunks):
        s = scores[parts_at[c], :]
        w = jnp.where(s > F32(0.5 * NEG_FILL), jnp.exp(s - top), 0.0)
        total = total + jnp.sum(w, axis=0, keepdims=True)
        parts.append(jnp.transpose(w.astype(BF16)))
    wt = jnp.concatenate(parts, axis=1)

    own_wt = jnp.transpose(jnp.where(own_mask, own_w, 0.0))
    nv = jnp.concatenate([nvbuf[b].astype(F32) for b in range(batch)], axis=0)
    own_acc = lax.dot_general(
        own_wt, nv, (((1,), (0,)), ((), ())), preferred_element_type=F32,
        precision=lax.Precision.HIGHEST,
    )

    for c in range(pairs):
        v = jnp.concatenate([vbuf[2 * c], vbuf[2 * c + 1]], axis=1)
        acc = jnp.dot(wt[2 * c * SLOT : (2 * c + 2) * SLOT, :], v, preferred_element_type=F32)
        for j in range(2):
            b = 2 * c + j
            part = acc[j * SLOT : (j + 1) * SLOT, j * width : (j + 1) * width]
            part = part + own_acc[b * SLOT : (b + 1) * SLOT, :]
            out_ref[pl.ds(b, heads, stride=batch), :] = part[:heads]

    lane_b = lax.broadcasted_iota(jnp.int32, (batch, lanes), 1)
    row_b = lax.broadcasted_iota(jnp.int32, (batch, lanes), 0)
    stats = jnp.zeros((batch, lanes), F32)
    for b in range(batch):
        m_b = pltpu.roll(top, (lanes - b * SLOT) % lanes, 1) if b else top
        l_b = pltpu.roll(total, (lanes + SLOT - b * SLOT) % lanes, 1) if b != 1 else total
        stats = jnp.where(row_b == b, jnp.where(lane_b < SLOT, m_b, l_b), stats)
    out_ref[heads * batch :, :] = stats
    wcopy.wait()


def balanced_sum(values):
    while len(values) > 1:
        values = [values[i] + values[i + 1] for i in range(0, len(values), 2)]
    return values[0]


def merge(parts, heads, batch):
    stats = [p[heads * batch :, :] for p in parts]
    top = functools.reduce(jnp.maximum, stats)
    factors = [jnp.exp(s - top) for s in stats]
    total = balanced_sum([s * pltpu.roll(f, SLOT, 1) for s, f in zip(stats, factors)])
    lane = lax.broadcasted_iota(jnp.int32, top.shape, 1)
    sums = []
    for h in range(heads):
        rows = slice(h * batch, (h + 1) * batch)
        sums.append(balanced_sum([p[rows, :] * f[:, h : h + 1] for p, f in zip(parts, factors)]))
    return sums, jnp.where(lane < SLOT, top, total)


def merge_kernel(*refs, heads, batch):
    out_ref = refs[-1]
    sums, stats = merge(refs[:-1], heads, batch)
    for h in range(heads):
        out_ref[h * batch : (h + 1) * batch, :] = sums[h]
    out_ref[heads * batch :, :] = stats


def project_kernel(*refs, heads, batch):
    w_ref, out_ref = refs[-2:]
    sums, stats = merge(refs[:-2], heads, batch)
    attended = jnp.concatenate(
        [(sums[h] / stats[:, SLOT + h : SLOT + h + 1]).astype(BF16) for h in range(heads)], axis=1
    )
    out_ref[...] = jnp.dot(attended, w_ref[...], preferred_element_type=F32)


def vmem(x):
    return pltpu.with_memory_space_constraint(x, pltpu.VMEM)


def in_vmem(count):
    return [pl.BlockSpec(memory_space=pltpu.VMEM)] * count


def exchange_steps(axis):
    size = lax.axis_size(axis)
    assert size & (size - 1) == 0
    steps, low = [], 1
    while low < size:
        steps.append([low, 2 * low, 3 * low] if 4 * low <= size else [low])
        low *= len(steps[-1]) + 1
    return steps


def gather_from(value, axis, distances, ring=False):
    size = lax.axis_size(axis)
    moves = [[(i, i ^ d) for i in range(size)] for d in distances]
    if ring and len(distances) == 3:
        low = distances[0]
        after = (1, 3, 0, 2)
        onward = [(i, i + low * (after[i // low % 4] - i // low % 4)) for i in range(size)]
        moves = [moves[2], onward, [(b, a) for a, b in onward]]
    return [value] + [lax.ppermute(value, axis, pairs) for pairs in moves]


def body(query, key_cache, value_cache, new_key, new_value, lengths, out_weight):
    seq_count = lax.axis_size("seq")
    batch, span, kv, width = key_cache.shape
    heads = query.shape[1]
    stretch = span * seq_count // 8
    rows = span * kv
    sizes = [rows * n // 16 for n in (4, 5, 7)]
    lanes = batch * SLOT
    packed_rows = heads * batch + batch
    dma = pltpu.SemaphoreType.DMA
    packed, weight = pl.pallas_call(
        functools.partial(attention_kernel, stretch=stretch, kv=kv, sizes=sizes),
        out_shape=[pltpu.VMEM((packed_rows, width), F32), pltpu.VMEM(out_weight.shape, BF16)],
        in_specs=[pl.BlockSpec(memory_space=pl.ANY)] * 7,
        out_specs=in_vmem(2),
        scratch_shapes=[
            pltpu.VMEM((2, rows, width), F32),
            pltpu.SMEM((batch,), jnp.int32),
            pltpu.VMEM((heads, batch, width), BF16),
            pltpu.VMEM((batch, kv, width), BF16),
            pltpu.VMEM((batch, kv, width), BF16),
            pltpu.VMEM((batch, rows, width), BF16),
            pltpu.VMEM((batch, rows, width), BF16),
            pltpu.VMEM((batch, max(sizes), width), BF16),
            pltpu.VMEM((batch, max(sizes), width), BF16),
            pltpu.VMEM((lanes, batch * width), BF16),
            pltpu.VMEM((lanes, width), BF16),
            pltpu.VMEM((2, heads * batch, width), F32),
            pltpu.VMEM((rows, lanes), F32),
            dma((len(sizes),)), dma, dma, dma, dma, dma, dma, pltpu.SemaphoreType.REGULAR,
        ],
        name="attention",
    )(
        lengths, jnp.transpose(query, (1, 0, 2)), new_key, new_value,
        key_cache.reshape(batch, rows, width), value_cache.reshape(batch, rows, width),
        out_weight,
    )
    steps = exchange_steps("seq")
    for distances in steps[:-1]:
        parts = gather_from(packed, "seq", distances, ring=True)
        packed = pl.pallas_call(
            functools.partial(merge_kernel, heads=heads, batch=batch),
            out_shape=pltpu.VMEM(packed.shape, F32),
            in_specs=in_vmem(len(parts)),
            out_specs=in_vmem(1)[0],
            name="merge",
        )(*map(vmem, parts))
    parts = gather_from(packed, "seq", steps[-1], ring=True)
    share = pl.pallas_call(
        functools.partial(project_kernel, heads=heads, batch=batch),
        out_shape=pltpu.VMEM((batch, out_weight.shape[1]), F32),
        in_specs=in_vmem(len(parts) + 1),
        out_specs=in_vmem(1)[0],
        name="project",
    )(*map(vmem, parts), vmem(weight))
    for distances in exchange_steps("head"):
        share = balanced_sum(gather_from(share, "head", distances))
    return share


def solution(mesh):
    placed = (
        P(None, "head", None),
        P(None, "seq", "head", None),
        P(None, "seq", "head", None),
        P(None, "head", None),
        P(None, "head", None),
        P(),
        P("head", "seq"),
    )
    return jax.shard_map(
        body, mesh=mesh, in_specs=placed, out_specs=P(None, "seq"), check_vma=False
    )
```

```python
import functools
import math

import jax
import jax.numpy as jnp
from jax import lax
from jax.experimental import pallas as pl
from jax.experimental.pallas import tpu as pltpu
from jax.sharding import PartitionSpec as P

THETA_BASE = 10000000.0
NEG_FILL = -1e30
RUN = 32
SLOT = 16
F32 = jnp.float32
BF16 = jnp.bfloat16


def frequencies(shape):
    width = shape[-1]
    half = width // 2
    lane = lax.broadcasted_iota(jnp.int32, shape, len(shape) - 1)
    index = jnp.where(lane < half, lane, lane - half).astype(F32)
    return jnp.exp(index * F32(-2.0 * math.log(THETA_BASE) / width))


def half_sign(shape):
    lane = lax.broadcasted_iota(jnp.int32, shape, len(shape) - 1)
    return jnp.where(lane < shape[-1] // 2, F32(-1.0), F32(1.0))


def rotate(values, cos_part, signed_sin):
    return values * cos_part + pltpu.roll(values, values.shape[-1] // 2, 1) * signed_sin


def rows_of_scalars(scalars, shape):
    row = lax.broadcasted_iota(jnp.int32, shape, 0)
    out = jnp.zeros(shape, scalars[0].dtype)
    for i, s in enumerate(scalars):
        out = jnp.where(row == i, s, out)
    return out


def attention_kernel(
    lens_hbm, q_hbm, nk_hbm, nv_hbm, k_hbm, v_hbm, w_hbm,
    out_ref, w_ref,
    tab, lens, qbuf, nkbuf, nvbuf, kbuf, vbuf, kcat0, kcat1, qbd, qin, qrot, scores,
    ksem, vsem, lsem, qsem, nksem, nvsem, wsem, order,
    *, stretch, kv, sizes,
):
    batch, rows, width = kbuf.shape
    heads = qbuf.shape[0]
    group = heads // kv
    lanes = batch * SLOT
    span = rows // kv
    chunks = len(sizes)
    parts_at = [slice(sum(sizes[:c]), sum(sizes[: c + 1])) for c in range(chunks)]
    pairs = batch // 2
    kcats = (kcat0, kcat1)

    def kcopy(c):
        part = pl.ds(parts_at[c].start, sizes[c])
        return pltpu.make_async_copy(k_hbm.at[:, part, :], kbuf.at[:, part, :], ksem.at[c])

    vcopy = pltpu.make_async_copy(v_hbm, vbuf, vsem)
    wcopy = pltpu.make_async_copy(w_hbm, w_ref, wsem)

    lcopy = pltpu.make_async_copy(lens_hbm, lens, lsem)
    qcopy = pltpu.make_async_copy(q_hbm, qbuf, qsem)
    nkcopy = pltpu.make_async_copy(nk_hbm, nkbuf, nksem)
    nvcopy = pltpu.make_async_copy(nv_hbm, nvbuf, nvsem)
    small = (lcopy, qcopy, nkcopy, nvcopy)
    for copy in small:
        copy.start()
    pl.semaphore_signal(order, 1)
    pl.semaphore_wait(order, 1)
    for c in range(chunks):
        kcopy(c).start()
    vcopy.start()

    place = lax.axis_index("seq").astype(jnp.int32)
    base = place * span
    key_stretch = base // stretch

    qbd[...] = jnp.zeros_like(qbd)
    qin[...] = jnp.zeros_like(qin)
    freq8 = frequencies((batch, width))
    sign8 = half_sign((batch, width))

    runs = span // RUN
    start = (base % stretch).astype(F32)
    far = start + (RUN * lax.broadcasted_iota(jnp.int32, (runs, width), 0)).astype(F32)
    far = far * frequencies((runs, width))
    far_c, far_s = jnp.cos(far), jnp.sin(far) * half_sign((runs, width))
    near = lax.broadcasted_iota(jnp.int32, (RUN, width), 0).astype(F32) * frequencies((RUN, width))
    near_c, near_signed = jnp.cos(near), jnp.sin(near) * half_sign((RUN, width))
    for i in range(runs):
        c_i, s_i = far_c[i : i + 1], far_s[i : i + 1]
        cos_part = c_i * near_c - s_i * near_signed
        sin_part = s_i * near_c + c_i * near_signed
        for j in range(kv):
            at = pl.ds(RUN * kv * i + j, RUN, stride=kv)
            tab[0, at, :] = cos_part
            tab[1, at, :] = sin_part

    for copy in small:
        copy.wait()
    picked, intra, limit = [], [], []
    for b in range(batch):
        p = lens[b]
        qc = p // stretch
        r = p - qc * stretch
        intra.append(r.astype(F32))
        inter = stretch + stretch // 2
        picked.append(
            jnp.where(key_stretch == qc, r, jnp.where(key_stretch == qc - 1, r + stretch, inter)).astype(F32)
        )
        limit.append((p - base) * kv)
    angle_p = rows_of_scalars(picked, (batch, width)) * freq8
    angle_r = rows_of_scalars(intra, (batch, width)) * freq8
    cp, sp = jnp.cos(angle_p), jnp.sin(angle_p) * sign8
    cr, sr = jnp.cos(angle_r), jnp.sin(angle_r) * sign8

    for h in range(heads):
        q = qbuf[h].astype(F32)
        at = slice(h * batch, (h + 1) * batch)
        qrot[0, at, :] = rotate(q, cp, sp)
        qrot[1, at, :] = rotate(q, cr, sr)
    for b in range(batch):
        mine = pl.ds(b, heads, stride=batch)
        at = slice(b * SLOT, b * SLOT + heads)
        qbd[at, b * width : (b + 1) * width] = qrot[0, mine, :].astype(BF16)
        qin[at, :] = qrot[1, mine, :].astype(BF16)

    scaling = F32(1.0 / math.sqrt(width))

    lane1 = lax.broadcasted_iota(jnp.int32, (1, lanes), 1)
    bound = jnp.zeros((1, lanes), jnp.int32)
    for b in range(batch):
        bound = jnp.where(lane1 // SLOT == b, limit[b], bound)
    lane_kv = jnp.minimum((lane1 % SLOT) // group, kv - 1)
    row8 = lax.broadcasted_iota(jnp.int32, (8, lanes), 0)
    bound8 = jnp.where(row8 % kv == lane_kv, bound - row8, -1)

    def rotate_keys(c):
        part = parts_at[c]
        for b in range(batch):
            k = kbuf[b, part, :]
            turned = pltpu.roll(k, width // 2, 1).astype(F32)
            k = k.astype(F32) * tab[0, part, :] + turned * tab[1, part, :]
            kcats[c % 2][b, : sizes[c], :] = k.astype(BF16)

    def score(c, top):
        half = sizes[c] // 2
        sums = []
        for part in (slice(0, half), slice(half, sizes[c])):
            keys = jnp.concatenate([kcats[c % 2][b, part, :] for b in range(batch)], axis=1)
            sums.append(lax.dot_general(
                keys, qbd[...], (((1,), (1,)), ((), ())), preferred_element_type=F32
            ))
        s = jnp.concatenate(sums, axis=0) * scaling
        s = s.reshape(sizes[c] // 8, 8, lanes)
        row = parts_at[c].start + 8 * lax.broadcasted_iota(jnp.int32, s.shape, 0)
        s = jnp.where(row < bound8[None], s, F32(NEG_FILL)).reshape(sizes[c], lanes)
        scores[parts_at[c], :] = s
        return jnp.maximum(top, jnp.max(s, axis=0, keepdims=True))

    for c in range(chunks):
        kcopy(c).wait()
        if c == chunks - 1:
            wcopy.start()
        rotate_keys(c)
        if c == 1:
            own_rows = batch * kv
            knew = jnp.concatenate(
                [rotate(nkbuf[b].astype(F32), cr[b : b + 1], sr[b : b + 1]) for b in range(batch)], axis=0
            ).astype(BF16)
            own_all = lax.dot_general(
                knew, qin[...], (((1,), (1,)), ((), ())), preferred_element_type=F32
            ) * scaling
            own_row = lax.broadcasted_iota(jnp.int32, (own_rows, lanes), 0)
            own_lane = lax.broadcasted_iota(jnp.int32, (own_rows, lanes), 1)
            own_kv = jnp.minimum((own_lane % SLOT) // group, kv - 1)
            own_mask = (own_row // kv == own_lane // SLOT) & (own_row % kv == own_kv)
            own = jnp.sum(jnp.where(own_mask, own_all, 0.0), axis=0, keepdims=True)
            first = place == 0
            own = jnp.where(first, own, F32(NEG_FILL))
            top = own
        if c:
            top = score(c - 1, top)
    vcopy.wait()
    top = score(chunks - 1, top)

    own_w = jnp.where(first, jnp.exp(own - top), 0.0)
    total = own_w
    parts = []
    for c in range(chunks):
        s = scores[parts_at[c], :]
        w = jnp.exp(s - jnp.maximum(top, F32(0.5 * NEG_FILL)))
        total = total + jnp.sum(w, axis=0, keepdims=True)
        parts.append(jnp.transpose(w.astype(BF16)))
    wt = jnp.concatenate(parts, axis=1)

    own_wt = jnp.transpose(jnp.where(own_mask, own_w, 0.0))
    nv = jnp.concatenate([nvbuf[b].astype(F32) for b in range(batch)], axis=0)
    own_acc = lax.dot_general(
        own_wt, nv, (((1,), (0,)), ((), ())), preferred_element_type=F32,
        precision=lax.Precision.HIGHEST,
    )

    for c in range(pairs):
        v = jnp.concatenate([vbuf[2 * c], vbuf[2 * c + 1]], axis=1)
        acc = jnp.dot(wt[2 * c * SLOT : (2 * c + 2) * SLOT, :], v, preferred_element_type=F32)
        for j in range(2):
            b = 2 * c + j
            part = acc[j * SLOT : (j + 1) * SLOT, j * width : (j + 1) * width]
            part = part + own_acc[b * SLOT : (b + 1) * SLOT, :]
            out_ref[pl.ds(b, heads, stride=batch), :] = part[:heads]

    lane_b = lax.broadcasted_iota(jnp.int32, (batch, lanes), 1)
    row_b = lax.broadcasted_iota(jnp.int32, (batch, lanes), 0)
    stats = jnp.zeros((batch, lanes), F32)
    for b in range(batch):
        m_b = pltpu.roll(top, (lanes - b * SLOT) % lanes, 1) if b else top
        l_b = pltpu.roll(total, (lanes + SLOT - b * SLOT) % lanes, 1) if b != 1 else total
        stats = jnp.where(row_b == b, jnp.where(lane_b < SLOT, m_b, l_b), stats)
    out_ref[heads * batch :, :] = stats
    wcopy.wait()


def balanced_sum(values):
    while len(values) > 1:
        values = [values[i] + values[i + 1] for i in range(0, len(values), 2)]
    return values[0]


def merge(parts, heads, batch):
    stats = [p[heads * batch :, :] for p in parts]
    top = functools.reduce(jnp.maximum, stats)
    factors = [jnp.exp(s - top) for s in stats]
    total = balanced_sum([s * pltpu.roll(f, SLOT, 1) for s, f in zip(stats, factors)])
    lane = lax.broadcasted_iota(jnp.int32, top.shape, 1)
    sums = []
    for h in range(heads):
        rows = slice(h * batch, (h + 1) * batch)
        sums.append(balanced_sum([p[rows, :] * f[:, h : h + 1] for p, f in zip(parts, factors)]))
    return sums, jnp.where(lane < SLOT, top, total)


def merge_kernel(*refs, heads, batch):
    out_ref = refs[-1]
    sums, stats = merge(refs[:-1], heads, batch)
    for h in range(heads):
        out_ref[h * batch : (h + 1) * batch, :] = sums[h]
    out_ref[heads * batch :, :] = stats


def project_kernel(*refs, heads, batch):
    w_ref, out_ref = refs[-2:]
    sums, stats = merge(refs[:-2], heads, batch)
    attended = jnp.concatenate(
        [(sums[h] / stats[:, SLOT + h : SLOT + h + 1]).astype(BF16) for h in range(heads)], axis=1
    )
    out_ref[...] = jnp.dot(attended, w_ref[...], preferred_element_type=F32)


def vmem(x):
    return pltpu.with_memory_space_constraint(x, pltpu.VMEM)


def in_vmem(count):
    return [pl.BlockSpec(memory_space=pltpu.VMEM)] * count


def exchange_steps(axis):
    size = lax.axis_size(axis)
    assert size & (size - 1) == 0
    steps, low = [], 1
    while low < size:
        steps.append([low, 2 * low, 3 * low] if 4 * low <= size else [low])
        low *= len(steps[-1]) + 1
    return steps


def gather_from(value, axis, distances, ring=False):
    size = lax.axis_size(axis)
    moves = [[(i, i ^ d) for i in range(size)] for d in distances]
    if ring and len(distances) == 3:
        low = distances[0]
        after = (1, 3, 0, 2)
        onward = [(i, i + low * (after[i // low % 4] - i // low % 4)) for i in range(size)]
        moves = [moves[2], onward, [(b, a) for a, b in onward]]
    return [value] + [lax.ppermute(value, axis, pairs) for pairs in moves]


def body(query, key_cache, value_cache, new_key, new_value, lengths, out_weight):
    seq_count = lax.axis_size("seq")
    batch, span, kv, width = key_cache.shape
    heads = query.shape[1]
    stretch = span * seq_count // 8
    rows = span * kv
    sizes = [rows * n // 16 for n in (4, 5, 7)]
    lanes = batch * SLOT
    packed_rows = heads * batch + batch
    dma = pltpu.SemaphoreType.DMA
    packed, weight = pl.pallas_call(
        functools.partial(attention_kernel, stretch=stretch, kv=kv, sizes=sizes),
        out_shape=[pltpu.VMEM((packed_rows, width), F32), pltpu.VMEM(out_weight.shape, BF16)],
        in_specs=[pl.BlockSpec(memory_space=pl.ANY)] * 7,
        out_specs=in_vmem(2),
        scratch_shapes=[
            pltpu.VMEM((2, rows, width), F32),
            pltpu.SMEM((batch,), jnp.int32),
            pltpu.VMEM((heads, batch, width), BF16),
            pltpu.VMEM((batch, kv, width), BF16),
            pltpu.VMEM((batch, kv, width), BF16),
            pltpu.VMEM((batch, rows, width), BF16),
            pltpu.VMEM((batch, rows, width), BF16),
            pltpu.VMEM((batch, max(sizes), width), BF16),
            pltpu.VMEM((batch, max(sizes), width), BF16),
            pltpu.VMEM((lanes, batch * width), BF16),
            pltpu.VMEM((lanes, width), BF16),
            pltpu.VMEM((2, heads * batch, width), F32),
            pltpu.VMEM((rows, lanes), F32),
            dma((len(sizes),)), dma, dma, dma, dma, dma, dma, pltpu.SemaphoreType.REGULAR,
        ],
        name="attention",
    )(
        lengths, jnp.transpose(query, (1, 0, 2)), new_key, new_value,
        key_cache.reshape(batch, rows, width), value_cache.reshape(batch, rows, width),
        out_weight,
    )
    steps = exchange_steps("seq")
    for distances in steps[:-1]:
        parts = gather_from(packed, "seq", distances, ring=True)
        packed = pl.pallas_call(
            functools.partial(merge_kernel, heads=heads, batch=batch),
            out_shape=pltpu.VMEM(packed.shape, F32),
            in_specs=in_vmem(len(parts)),
            out_specs=in_vmem(1)[0],
            name="merge",
        )(*map(vmem, parts))
    parts = gather_from(packed, "seq", steps[-1], ring=True)
    share = pl.pallas_call(
        functools.partial(project_kernel, heads=heads, batch=batch),
        out_shape=pltpu.VMEM((batch, out_weight.shape[1]), F32),
        in_specs=in_vmem(len(parts) + 1),
        out_specs=in_vmem(1)[0],
        name="project",
    )(*map(vmem, parts), vmem(weight))
    for distances in exchange_steps("head"):
        share = balanced_sum(gather_from(share, "head", distances))
    return share


def solution(mesh):
    placed = (
        P(None, "head", None),
        P(None, "seq", "head", None),
        P(None, "seq", "head", None),
        P(None, "head", None),
        P(None, "head", None),
        P(),
        P("head", "seq"),
    )
    return jax.shard_map(
        body, mesh=mesh, in_specs=placed, out_specs=P(None, "seq"), check_vma=False
    )
```

```python
import functools
import math

import jax
import jax.numpy as jnp
from jax import lax
from jax.experimental import pallas as pl
from jax.experimental.pallas import tpu as pltpu
from jax.sharding import PartitionSpec as P

THETA_BASE = 10000000.0
NEG_FILL = -1e30
RUN = 32
SLOT = 16
F32 = jnp.float32
BF16 = jnp.bfloat16


def frequencies(shape):
    width = shape[-1]
    half = width // 2
    lane = lax.broadcasted_iota(jnp.int32, shape, len(shape) - 1)
    index = jnp.where(lane < half, lane, lane - half).astype(F32)
    return jnp.exp(index * F32(-2.0 * math.log(THETA_BASE) / width))


def half_sign(shape):
    lane = lax.broadcasted_iota(jnp.int32, shape, len(shape) - 1)
    return jnp.where(lane < shape[-1] // 2, F32(-1.0), F32(1.0))


def rotate(values, cos_part, signed_sin):
    return values * cos_part + pltpu.roll(values, values.shape[-1] // 2, 1) * signed_sin


def rows_of_scalars(scalars, shape):
    row = lax.broadcasted_iota(jnp.int32, shape, 0)
    out = jnp.zeros(shape, scalars[0].dtype)
    for i, s in enumerate(scalars):
        out = jnp.where(row == i, s, out)
    return out


def attention_kernel(
    lens_hbm, q_hbm, nk_hbm, nv_hbm, k_hbm, v_hbm, w_hbm,
    out_ref, w_ref,
    tab, lens, qbuf, nkbuf, nvbuf, kbuf, vbuf, kcat0, kcat1, qbd, qin, qrot, scores,
    ksem, vsem, lsem, qsem, nksem, nvsem, wsem, order,
    *, stretch, kv, sizes,
):
    batch, rows, width = kbuf.shape
    heads = qbuf.shape[0]
    group = heads // kv
    lanes = batch * SLOT
    span = rows // kv
    chunks = len(sizes)
    parts_at = [slice(sum(sizes[:c]), sum(sizes[: c + 1])) for c in range(chunks)]
    pairs = batch // 2
    kcats = (kcat0, kcat1)

    def kcopy(c):
        part = pl.ds(parts_at[c].start, sizes[c])
        return pltpu.make_async_copy(k_hbm.at[:, part, :], kbuf.at[:, part, :], ksem.at[c])

    vcopy = pltpu.make_async_copy(v_hbm, vbuf, vsem)
    wcopy = pltpu.make_async_copy(w_hbm, w_ref, wsem)

    lcopy = pltpu.make_async_copy(lens_hbm, lens, lsem)
    qcopy = pltpu.make_async_copy(q_hbm, qbuf, qsem)
    nkcopy = pltpu.make_async_copy(nk_hbm, nkbuf, nksem)
    nvcopy = pltpu.make_async_copy(nv_hbm, nvbuf, nvsem)
    small = (lcopy, qcopy, nkcopy, nvcopy)
    for copy in small:
        copy.start()
    pl.semaphore_signal(order, 1)
    pl.semaphore_wait(order, 1)
    for c in range(chunks):
        kcopy(c).start()
    vcopy.start()

    place = lax.axis_index("seq").astype(jnp.int32)
    base = place * span
    key_stretch = base // stretch

    qin[...] = jnp.zeros_like(qin)
    freq8 = frequencies((batch, width))
    sign8 = half_sign((batch, width))

    runs = span // RUN
    start = (base % stretch).astype(F32)
    far = start + (RUN * lax.broadcasted_iota(jnp.int32, (runs, width), 0)).astype(F32)
    far = far * frequencies((runs, width))
    far_c, far_s = jnp.cos(far), jnp.sin(far) * half_sign((runs, width))
    near = lax.broadcasted_iota(jnp.int32, (RUN, width), 0).astype(F32) * frequencies((RUN, width))
    near_c, near_signed = jnp.cos(near), jnp.sin(near) * half_sign((RUN, width))
    for i in range(runs):
        c_i, s_i = far_c[i : i + 1], far_s[i : i + 1]
        cos_part = c_i * near_c - s_i * near_signed
        sin_part = s_i * near_c + c_i * near_signed
        for j in range(kv):
            at = pl.ds(RUN * kv * i + j, RUN, stride=kv)
            tab[0, at, :] = cos_part
            tab[1, at, :] = sin_part

    for copy in small:
        copy.wait()
    picked, intra, limit = [], [], []
    for b in range(batch):
        p = lens[b]
        qc = p // stretch
        r = p - qc * stretch
        intra.append(r.astype(F32))
        inter = stretch + stretch // 2
        picked.append(
            jnp.where(key_stretch == qc, r, jnp.where(key_stretch == qc - 1, r + stretch, inter)).astype(F32)
        )
        limit.append((p - base) * kv)
    angle_p = rows_of_scalars(picked, (batch, width)) * freq8
    angle_r = rows_of_scalars(intra, (batch, width)) * freq8
    cp, sp = jnp.cos(angle_p), jnp.sin(angle_p) * sign8
    cr, sr = jnp.cos(angle_r), jnp.sin(angle_r) * sign8

    for h in range(heads):
        q = qbuf[h].astype(F32)
        at = slice(h * batch, (h + 1) * batch)
        qrot[0, at, :] = rotate(q, cp, sp)
        qrot[1, at, :] = rotate(q, cr, sr)
    for b in range(batch):
        mine = pl.ds(b, heads, stride=batch)
        at = slice(b * SLOT, b * SLOT + heads)
        qin[0, at, :] = qrot[0, mine, :].astype(BF16)
        qin[1, at, :] = qrot[1, mine, :].astype(BF16)
    turned_q = jnp.transpose(qin[0])
    q_lane = lax.broadcasted_iota(jnp.int32, (width, lanes), 1) // SLOT
    for b in range(batch):
        qbd[b * width : (b + 1) * width, :] = jnp.where(q_lane == b, turned_q, jnp.zeros_like(turned_q))

    scaling = F32(1.0 / math.sqrt(width))

    lane1 = lax.broadcasted_iota(jnp.int32, (1, lanes), 1)
    bound = jnp.zeros((1, lanes), jnp.int32)
    for b in range(batch):
        bound = jnp.where(lane1 // SLOT == b, limit[b], bound)
    lane_kv = jnp.minimum((lane1 % SLOT) // group, kv - 1)
    row8 = lax.broadcasted_iota(jnp.int32, (8, lanes), 0)
    bound8 = jnp.where(row8 % kv == lane_kv, bound - row8, -1)

    def rotate_keys(c):
        part = parts_at[c]
        for b in range(batch):
            k = kbuf[b, part, :]
            turned = pltpu.roll(k, width // 2, 1).astype(F32)
            k = k.astype(F32) * tab[0, part, :] + turned * tab[1, part, :]
            kcats[c % 2][b, : sizes[c], :] = k.astype(BF16)

    def score(c, top):
        half = sizes[c] // 2
        sums = []
        for part in (slice(0, half), slice(half, sizes[c])):
            keys = jnp.concatenate([kcats[c % 2][b, part, :] for b in range(batch)], axis=1)
            sums.append(jnp.dot(keys, qbd[...], preferred_element_type=F32))
        s = jnp.concatenate(sums, axis=0) * scaling
        s = s.reshape(sizes[c] // 8, 8, lanes)
        row = parts_at[c].start + 8 * lax.broadcasted_iota(jnp.int32, s.shape, 0)
        s = jnp.where(row < bound8[None], s, F32(NEG_FILL)).reshape(sizes[c], lanes)
        scores[parts_at[c], :] = s
        return jnp.maximum(top, jnp.max(s, axis=0, keepdims=True))

    for c in range(chunks):
        kcopy(c).wait()
        if c == chunks - 1:
            wcopy.start()
        rotate_keys(c)
        if c == 1:
            own_rows = batch * kv
            knew = jnp.concatenate(
                [rotate(nkbuf[b].astype(F32), cr[b : b + 1], sr[b : b + 1]) for b in range(batch)], axis=0
            ).astype(BF16)
            own_all = lax.dot_general(
                knew, qin[1], (((1,), (1,)), ((), ())), preferred_element_type=F32
            ) * scaling
            own_row = lax.broadcasted_iota(jnp.int32, (own_rows, lanes), 0)
            own_lane = lax.broadcasted_iota(jnp.int32, (own_rows, lanes), 1)
            own_kv = jnp.minimum((own_lane % SLOT) // group, kv - 1)
            own_mask = (own_row // kv == own_lane // SLOT) & (own_row % kv == own_kv)
            own = jnp.sum(jnp.where(own_mask, own_all, 0.0), axis=0, keepdims=True)
            first = place == 0
            own = jnp.where(first, own, F32(NEG_FILL))
            top = own
        if c:
            top = score(c - 1, top)
    vcopy.wait()
    top = score(chunks - 1, top)

    own_w = jnp.where(first, jnp.exp(own - top), 0.0)
    total = own_w
    parts = []
    for c in range(chunks):
        s = scores[parts_at[c], :]
        w = jnp.exp(s - jnp.maximum(top, F32(0.5 * NEG_FILL)))
        total = total + jnp.sum(w, axis=0, keepdims=True)
        parts.append(jnp.transpose(w.astype(BF16)))
    wt = jnp.concatenate(parts, axis=1)

    own_wt = jnp.transpose(jnp.where(own_mask, own_w, 0.0))
    nv = jnp.concatenate([nvbuf[b].astype(F32) for b in range(batch)], axis=0)
    own_acc = lax.dot_general(
        own_wt, nv, (((1,), (0,)), ((), ())), preferred_element_type=F32,
        precision=lax.Precision.HIGHEST,
    )

    for c in range(pairs):
        v = jnp.concatenate([vbuf[2 * c], vbuf[2 * c + 1]], axis=1)
        acc = jnp.dot(wt[2 * c * SLOT : (2 * c + 2) * SLOT, :], v, preferred_element_type=F32)
        for j in range(2):
            b = 2 * c + j
            part = acc[j * SLOT : (j + 1) * SLOT, j * width : (j + 1) * width]
            part = part + own_acc[b * SLOT : (b + 1) * SLOT, :]
            out_ref[pl.ds(b, heads, stride=batch), :] = part[:heads]

    lane_b = lax.broadcasted_iota(jnp.int32, (batch, lanes), 1)
    row_b = lax.broadcasted_iota(jnp.int32, (batch, lanes), 0)
    stats = jnp.zeros((batch, lanes), F32)
    for b in range(batch):
        m_b = pltpu.roll(top, (lanes - b * SLOT) % lanes, 1) if b else top
        l_b = pltpu.roll(total, (lanes + SLOT - b * SLOT) % lanes, 1) if b != 1 else total
        stats = jnp.where(row_b == b, jnp.where(lane_b < SLOT, m_b, l_b), stats)
    out_ref[heads * batch :, :] = stats
    wcopy.wait()


def balanced_sum(values):
    while len(values) > 1:
        values = [values[i] + values[i + 1] for i in range(0, len(values), 2)]
    return values[0]


def merge(parts, heads, batch):
    stats = [p[heads * batch :, :] for p in parts]
    top = functools.reduce(jnp.maximum, stats)
    factors = [jnp.exp(s - top) for s in stats]
    total = balanced_sum([s * pltpu.roll(f, SLOT, 1) for s, f in zip(stats, factors)])
    lane = lax.broadcasted_iota(jnp.int32, top.shape, 1)
    sums = []
    for h in range(heads):
        rows = slice(h * batch, (h + 1) * batch)
        sums.append(balanced_sum([p[rows, :] * f[:, h : h + 1] for p, f in zip(parts, factors)]))
    return sums, jnp.where(lane < SLOT, top, total)


def merge_kernel(*refs, heads, batch):
    out_ref = refs[-1]
    sums, stats = merge(refs[:-1], heads, batch)
    for h in range(heads):
        out_ref[h * batch : (h + 1) * batch, :] = sums[h]
    out_ref[heads * batch :, :] = stats


def project_kernel(*refs, heads, batch):
    w_ref, out_ref = refs[-2:]
    sums, stats = merge(refs[:-2], heads, batch)
    attended = jnp.concatenate(
        [(sums[h] / stats[:, SLOT + h : SLOT + h + 1]).astype(BF16) for h in range(heads)], axis=1
    )
    out_ref[...] = jnp.dot(attended, w_ref[...], preferred_element_type=F32)


def vmem(x):
    return pltpu.with_memory_space_constraint(x, pltpu.VMEM)


def in_vmem(count):
    return [pl.BlockSpec(memory_space=pltpu.VMEM)] * count


def exchange_steps(axis):
    size = lax.axis_size(axis)
    assert size & (size - 1) == 0
    steps, low = [], 1
    while low < size:
        steps.append([low, 2 * low, 3 * low] if 4 * low <= size else [low])
        low *= len(steps[-1]) + 1
    return steps


def gather_from(value, axis, distances, ring=False):
    size = lax.axis_size(axis)
    moves = [[(i, i ^ d) for i in range(size)] for d in distances]
    if ring and len(distances) == 3:
        low = distances[0]
        after = (1, 3, 0, 2)
        onward = [(i, i + low * (after[i // low % 4] - i // low % 4)) for i in range(size)]
        moves = [moves[2], onward, [(b, a) for a, b in onward]]
    return [value] + [lax.ppermute(value, axis, pairs) for pairs in moves]


def body(query, key_cache, value_cache, new_key, new_value, lengths, out_weight):
    seq_count = lax.axis_size("seq")
    batch, span, kv, width = key_cache.shape
    heads = query.shape[1]
    stretch = span * seq_count // 8
    rows = span * kv
    sizes = [rows * n // 16 for n in (4, 5, 7)]
    lanes = batch * SLOT
    packed_rows = heads * batch + batch
    dma = pltpu.SemaphoreType.DMA
    packed, weight = pl.pallas_call(
        functools.partial(attention_kernel, stretch=stretch, kv=kv, sizes=sizes),
        out_shape=[pltpu.VMEM((packed_rows, width), F32), pltpu.VMEM(out_weight.shape, BF16)],
        in_specs=[pl.BlockSpec(memory_space=pl.ANY)] * 7,
        out_specs=in_vmem(2),
        scratch_shapes=[
            pltpu.VMEM((2, rows, width), F32),
            pltpu.SMEM((batch,), jnp.int32),
            pltpu.VMEM((heads, batch, width), BF16),
            pltpu.VMEM((batch, kv, width), BF16),
            pltpu.VMEM((batch, kv, width), BF16),
            pltpu.VMEM((batch, rows, width), BF16),
            pltpu.VMEM((batch, rows, width), BF16),
            pltpu.VMEM((batch, max(sizes), width), BF16),
            pltpu.VMEM((batch, max(sizes), width), BF16),
            pltpu.VMEM((batch * width, lanes), BF16),
            pltpu.VMEM((2, lanes, width), BF16),
            pltpu.VMEM((2, heads * batch, width), F32),
            pltpu.VMEM((rows, lanes), F32),
            dma((len(sizes),)), dma, dma, dma, dma, dma, dma, pltpu.SemaphoreType.REGULAR,
        ],
        name="attention",
    )(
        lengths, jnp.transpose(query, (1, 0, 2)), new_key, new_value,
        key_cache.reshape(batch, rows, width), value_cache.reshape(batch, rows, width),
        out_weight,
    )
    steps = exchange_steps("seq")
    for distances in steps[:-1]:
        parts = gather_from(packed, "seq", distances, ring=True)
        packed = pl.pallas_call(
            functools.partial(merge_kernel, heads=heads, batch=batch),
            out_shape=pltpu.VMEM(packed.shape, F32),
            in_specs=in_vmem(len(parts)),
            out_specs=in_vmem(1)[0],
            name="merge",
        )(*map(vmem, parts))
    parts = gather_from(packed, "seq", steps[-1], ring=True)
    share = pl.pallas_call(
        functools.partial(project_kernel, heads=heads, batch=batch),
        out_shape=pltpu.VMEM((batch, out_weight.shape[1]), F32),
        in_specs=in_vmem(len(parts) + 1),
        out_specs=in_vmem(1)[0],
        name="project",
    )(*map(vmem, parts), vmem(weight))
    for distances in exchange_steps("head"):
        share = balanced_sum(gather_from(share, "head", distances))
    return share


def solution(mesh):
    placed = (
        P(None, "head", None),
        P(None, "seq", "head", None),
        P(None, "seq", "head", None),
        P(None, "head", None),
        P(None, "head", None),
        P(),
        P("head", "seq"),
    )
    return jax.shard_map(
        body, mesh=mesh, in_specs=placed, out_specs=P(None, "seq"), check_vma=False
    )
```

```python
import functools
import math

import jax
import jax.numpy as jnp
from jax import lax
from jax.experimental import pallas as pl
from jax.experimental.pallas import tpu as pltpu
from jax.sharding import PartitionSpec as P

THETA_BASE = 10000000.0
NEG_FILL = -1e30
RUN = 32
SLOT = 16
F32 = jnp.float32
BF16 = jnp.bfloat16


def frequencies(shape):
    width = shape[-1]
    half = width // 2
    lane = lax.broadcasted_iota(jnp.int32, shape, len(shape) - 1)
    index = jnp.where(lane < half, lane, lane - half).astype(F32)
    return jnp.exp(index * F32(-2.0 * math.log(THETA_BASE) / width))


def half_sign(shape):
    lane = lax.broadcasted_iota(jnp.int32, shape, len(shape) - 1)
    return jnp.where(lane < shape[-1] // 2, F32(-1.0), F32(1.0))


def rotate(values, cos_part, signed_sin):
    return values * cos_part + pltpu.roll(values, values.shape[-1] // 2, 1) * signed_sin


def rows_of_scalars(scalars, shape):
    row = lax.broadcasted_iota(jnp.int32, shape, 0)
    out = jnp.zeros(shape, scalars[0].dtype)
    for i, s in enumerate(scalars):
        out = jnp.where(row == i, s, out)
    return out


def attention_kernel(
    lens_hbm, q_hbm, nk_hbm, nv_hbm, k_hbm, v_hbm, w_hbm,
    out_ref, w_ref,
    tab, lens, qbuf, nkbuf, nvbuf, kbuf, vbuf, kcat0, kcat1, qbd, qin, qrot, scores,
    ksem, vsem, lsem, qsem, nksem, nvsem, wsem, order,
    *, stretch, kv, sizes,
):
    batch, rows, width = kbuf.shape
    heads = qbuf.shape[0]
    group = heads // kv
    lanes = batch * SLOT
    span = rows // kv
    chunks = len(sizes)
    parts_at = [slice(sum(sizes[:c]), sum(sizes[: c + 1])) for c in range(chunks)]
    pairs = batch // 2
    kcats = (kcat0, kcat1)

    def kcopy(c):
        part = pl.ds(parts_at[c].start, sizes[c])
        return pltpu.make_async_copy(k_hbm.at[:, part, :], kbuf.at[:, part, :], ksem.at[c])

    vcopy = pltpu.make_async_copy(v_hbm, vbuf, vsem)
    wcopy = pltpu.make_async_copy(w_hbm, w_ref, wsem)

    lcopy = pltpu.make_async_copy(lens_hbm, lens, lsem)
    qcopy = pltpu.make_async_copy(q_hbm, qbuf, qsem)
    nkcopy = pltpu.make_async_copy(nk_hbm, nkbuf, nksem)
    nvcopy = pltpu.make_async_copy(nv_hbm, nvbuf, nvsem)
    small = (lcopy, qcopy, nkcopy, nvcopy)
    for copy in small:
        copy.start()
    pl.semaphore_signal(order, 1)
    pl.semaphore_wait(order, 1)
    for c in range(chunks):
        kcopy(c).start()
    vcopy.start()

    place = lax.axis_index("seq").astype(jnp.int32)
    base = place * span
    key_stretch = base // stretch

    qin[...] = jnp.zeros_like(qin)
    freq8 = frequencies((batch, width))
    sign8 = half_sign((batch, width))

    runs = span // RUN
    start = (base % stretch).astype(F32)
    far = start + (RUN * lax.broadcasted_iota(jnp.int32, (runs, width), 0)).astype(F32)
    far = far * frequencies((runs, width))
    far_c, far_s = jnp.cos(far), jnp.sin(far) * half_sign((runs, width))
    near = lax.broadcasted_iota(jnp.int32, (RUN, width), 0).astype(F32) * frequencies((RUN, width))
    near_c, near_signed = jnp.cos(near), jnp.sin(near) * half_sign((RUN, width))
    for i in range(runs):
        c_i, s_i = far_c[i : i + 1], far_s[i : i + 1]
        cos_part = c_i * near_c - s_i * near_signed
        sin_part = s_i * near_c + c_i * near_signed
        for j in range(kv):
            at = pl.ds(RUN * kv * i + j, RUN, stride=kv)
            tab[0, at, :] = cos_part
            tab[1, at, :] = sin_part

    for copy in small:
        copy.wait()
    picked, intra, limit = [], [], []
    for b in range(batch):
        p = lens[b]
        qc = p // stretch
        r = p - qc * stretch
        intra.append(r.astype(F32))
        inter = stretch + stretch // 2
        picked.append(
            jnp.where(key_stretch == qc, r, jnp.where(key_stretch == qc - 1, r + stretch, inter)).astype(F32)
        )
        limit.append((p - base) * kv)
    angle_p = rows_of_scalars(picked, (batch, width)) * freq8
    angle_r = rows_of_scalars(intra, (batch, width)) * freq8
    cp, sp = jnp.cos(angle_p), jnp.sin(angle_p) * sign8
    cr, sr = jnp.cos(angle_r), jnp.sin(angle_r) * sign8

    for h in range(heads):
        q = qbuf[h].astype(F32)
        at = slice(h * batch, (h + 1) * batch)
        qrot[0, at, :] = rotate(q, cp, sp)
        qrot[1, at, :] = rotate(q, cr, sr)
    for b in range(batch):
        mine = pl.ds(b, heads, stride=batch)
        at = slice(b * SLOT, b * SLOT + heads)
        qin[0, at, :] = qrot[0, mine, :].astype(BF16)
        qin[1, at, :] = qrot[1, mine, :].astype(BF16)
    turned_q = jnp.transpose(qin[0])
    q_lane = lax.broadcasted_iota(jnp.int32, (width, lanes), 1) // SLOT
    for b in range(batch):
        qbd[b * width : (b + 1) * width, :] = jnp.where(q_lane == b, turned_q, jnp.zeros_like(turned_q))

    scaling = F32(1.0 / math.sqrt(width))

    lane1 = lax.broadcasted_iota(jnp.int32, (1, lanes), 1)
    bound = jnp.zeros((1, lanes), jnp.int32)
    for b in range(batch):
        bound = jnp.where(lane1 // SLOT == b, limit[b], bound)
    lane_kv = jnp.minimum((lane1 % SLOT) // group, kv - 1)
    row8 = lax.broadcasted_iota(jnp.int32, (8, lanes), 0)
    bound8 = jnp.where(row8 % kv == lane_kv, bound - row8, -1)

    def rotate_keys(c):
        part = parts_at[c]
        for b in range(batch):
            k = kbuf[b, part, :]
            turned = pltpu.roll(k, width // 2, 1).astype(F32)
            k = k.astype(F32) * tab[0, part, :] + turned * tab[1, part, :]
            kcats[c % 2][b, : sizes[c], :] = k.astype(BF16)

    def score(c, top):
        half = sizes[c] // 2
        sums = []
        for part in (slice(0, half), slice(half, sizes[c])):
            keys = jnp.concatenate([kcats[c % 2][b, part, :] for b in range(batch)], axis=1)
            sums.append(jnp.dot(keys, qbd[...], preferred_element_type=F32))
        s = jnp.concatenate(sums, axis=0) * scaling
        s = s.reshape(sizes[c] // 8, 8, lanes)
        row = parts_at[c].start + 8 * lax.broadcasted_iota(jnp.int32, s.shape, 0)
        s = jnp.where(row < bound8[None], s, F32(NEG_FILL)).reshape(sizes[c], lanes)
        scores[parts_at[c], :] = s
        return jnp.maximum(top, jnp.max(s, axis=0, keepdims=True))

    for c in range(chunks):
        kcopy(c).wait()
        if c == chunks - 1:
            wcopy.start()
        rotate_keys(c)
        if c == 1:
            own_rows = batch * kv
            knew = jnp.concatenate(
                [rotate(nkbuf[b].astype(F32), cr[b : b + 1], sr[b : b + 1]) for b in range(batch)], axis=0
            ).astype(BF16)
            own_all = lax.dot_general(
                knew, qin[1], (((1,), (1,)), ((), ())), preferred_element_type=F32
            ) * scaling
            own_row = lax.broadcasted_iota(jnp.int32, (own_rows, lanes), 0)
            own_lane = lax.broadcasted_iota(jnp.int32, (own_rows, lanes), 1)
            own_kv = jnp.minimum((own_lane % SLOT) // group, kv - 1)
            own_mask = (own_row // kv == own_lane // SLOT) & (own_row % kv == own_kv)
            own = jnp.sum(jnp.where(own_mask, own_all, 0.0), axis=0, keepdims=True)
            first = place == 0
            own = jnp.where(first, own, F32(NEG_FILL))
            top = own
        if c:
            top = score(c - 1, top)
    vcopy.wait()
    top = score(chunks - 1, top)

    own_w = jnp.where(first, jnp.exp(own - top), 0.0)
    total = own_w
    parts = []
    for c in range(chunks):
        s = scores[parts_at[c], :]
        w = jnp.exp(s - jnp.maximum(top, F32(0.5 * NEG_FILL)))
        total = total + jnp.sum(w, axis=0, keepdims=True)
        parts.append(jnp.transpose(w.astype(BF16)))
    wt = jnp.concatenate(parts, axis=1)

    own_wt = jnp.transpose(jnp.where(own_mask, own_w, 0.0))
    nv = jnp.concatenate([nvbuf[b].astype(F32) for b in range(batch)], axis=0)
    own_acc = lax.dot_general(
        own_wt, nv, (((1,), (0,)), ((), ())), preferred_element_type=F32,
        precision=lax.Precision.HIGHEST,
    )

    for c in range(pairs):
        v = jnp.concatenate([vbuf[2 * c], vbuf[2 * c + 1]], axis=1)
        acc = jnp.dot(wt[2 * c * SLOT : (2 * c + 2) * SLOT, :], v, preferred_element_type=F32)
        for j in range(2):
            b = 2 * c + j
            part = acc[j * SLOT : (j + 1) * SLOT, j * width : (j + 1) * width]
            part = part + own_acc[b * SLOT : (b + 1) * SLOT, :]
            out_ref[pl.ds(b, heads, stride=batch), :] = part[:heads]

    lane_b = lax.broadcasted_iota(jnp.int32, (batch, lanes), 1)
    row_b = lax.broadcasted_iota(jnp.int32, (batch, lanes), 0)
    stats = jnp.zeros((batch, lanes), F32)
    for b in range(batch):
        m_b = pltpu.roll(top, (lanes - b * SLOT) % lanes, 1) if b else top
        l_b = pltpu.roll(total, (lanes + SLOT - b * SLOT) % lanes, 1) if b != 1 else total
        stats = jnp.where(row_b == b, jnp.where(lane_b < SLOT, m_b, l_b), stats)
    out_ref[heads * batch :, :] = stats
    wcopy.wait()


def balanced_sum(values):
    while len(values) > 1:
        values = [values[i] + values[i + 1] for i in range(0, len(values), 2)]
    return values[0]


def merge(parts, heads, batch):
    stats = [p[heads * batch :, :] for p in parts]
    top = functools.reduce(jnp.maximum, stats)
    factors = [jnp.exp(s - top) for s in stats]
    total = balanced_sum([s * pltpu.roll(f, SLOT, 1) for s, f in zip(stats, factors)])
    lane = lax.broadcasted_iota(jnp.int32, top.shape, 1)
    sums = []
    for h in range(heads):
        rows = slice(h * batch, (h + 1) * batch)
        sums.append(balanced_sum([p[rows, :] * f[:, h : h + 1] for p, f in zip(parts, factors)]))
    return sums, jnp.where(lane < SLOT, top, total)


def merge_kernel(*refs, heads, batch):
    out_ref = refs[-1]
    sums, stats = merge(refs[:-1], heads, batch)
    for h in range(heads):
        out_ref[h * batch : (h + 1) * batch, :] = sums[h]
    out_ref[heads * batch :, :] = stats


def project_kernel(*refs, heads, batch):
    w_ref, out_ref = refs[-2:]
    sums, stats = merge(refs[:-2], heads, batch)
    inverse = 1.0 / stats
    attended = jnp.concatenate(
        [(sums[h] * inverse[:, SLOT + h : SLOT + h + 1]).astype(BF16) for h in range(heads)], axis=1
    )
    out_ref[...] = jnp.dot(attended, w_ref[...], preferred_element_type=F32)


def vmem(x):
    return pltpu.with_memory_space_constraint(x, pltpu.VMEM)


def in_vmem(count):
    return [pl.BlockSpec(memory_space=pltpu.VMEM)] * count


def exchange_steps(axis):
    size = lax.axis_size(axis)
    assert size & (size - 1) == 0
    steps, low = [], 1
    while low < size:
        steps.append([low, 2 * low, 3 * low] if 4 * low <= size else [low])
        low *= len(steps[-1]) + 1
    return steps


def gather_from(value, axis, distances, ring=False):
    size = lax.axis_size(axis)
    moves = [[(i, i ^ d) for i in range(size)] for d in distances]
    if ring and len(distances) == 3:
        low = distances[0]
        after = (1, 3, 0, 2)
        onward = [(i, i + low * (after[i // low % 4] - i // low % 4)) for i in range(size)]
        moves = [moves[2], onward, [(b, a) for a, b in onward]]
    return [value] + [lax.ppermute(value, axis, pairs) for pairs in moves]


def body(query, key_cache, value_cache, new_key, new_value, lengths, out_weight):
    seq_count = lax.axis_size("seq")
    batch, span, kv, width = key_cache.shape
    heads = query.shape[1]
    stretch = span * seq_count // 8
    rows = span * kv
    sizes = [rows * n // 16 for n in (4, 5, 7)]
    lanes = batch * SLOT
    packed_rows = heads * batch + batch
    dma = pltpu.SemaphoreType.DMA
    packed, weight = pl.pallas_call(
        functools.partial(attention_kernel, stretch=stretch, kv=kv, sizes=sizes),
        out_shape=[pltpu.VMEM((packed_rows, width), F32), pltpu.VMEM(out_weight.shape, BF16)],
        in_specs=[pl.BlockSpec(memory_space=pl.ANY)] * 7,
        out_specs=in_vmem(2),
        scratch_shapes=[
            pltpu.VMEM((2, rows, width), F32),
            pltpu.SMEM((batch,), jnp.int32),
            pltpu.VMEM((heads, batch, width), BF16),
            pltpu.VMEM((batch, kv, width), BF16),
            pltpu.VMEM((batch, kv, width), BF16),
            pltpu.VMEM((batch, rows, width), BF16),
            pltpu.VMEM((batch, rows, width), BF16),
            pltpu.VMEM((batch, max(sizes), width), BF16),
            pltpu.VMEM((batch, max(sizes), width), BF16),
            pltpu.VMEM((batch * width, lanes), BF16),
            pltpu.VMEM((2, lanes, width), BF16),
            pltpu.VMEM((2, heads * batch, width), F32),
            pltpu.VMEM((rows, lanes), F32),
            dma((len(sizes),)), dma, dma, dma, dma, dma, dma, pltpu.SemaphoreType.REGULAR,
        ],
        name="attention",
    )(
        lengths, jnp.transpose(query, (1, 0, 2)), new_key, new_value,
        key_cache.reshape(batch, rows, width), value_cache.reshape(batch, rows, width),
        out_weight,
    )
    steps = exchange_steps("seq")
    for distances in steps[:-1]:
        parts = gather_from(packed, "seq", distances, ring=True)
        packed = pl.pallas_call(
            functools.partial(merge_kernel, heads=heads, batch=batch),
            out_shape=pltpu.VMEM(packed.shape, F32),
            in_specs=in_vmem(len(parts)),
            out_specs=in_vmem(1)[0],
            name="merge",
        )(*map(vmem, parts))
    parts = gather_from(packed, "seq", steps[-1], ring=True)
    share = pl.pallas_call(
        functools.partial(project_kernel, heads=heads, batch=batch),
        out_shape=pltpu.VMEM((batch, out_weight.shape[1]), F32),
        in_specs=in_vmem(len(parts) + 1),
        out_specs=in_vmem(1)[0],
        name="project",
    )(*map(vmem, parts), vmem(weight))
    for distances in exchange_steps("head"):
        share = balanced_sum(gather_from(share, "head", distances))
    return share


def solution(mesh):
    placed = (
        P(None, "head", None),
        P(None, "seq", "head", None),
        P(None, "seq", "head", None),
        P(None, "head", None),
        P(None, "head", None),
        P(),
        P("head", "seq"),
    )
    return jax.shard_map(
        body, mesh=mesh, in_specs=placed, out_specs=P(None, "seq"), check_vma=False
    )
```
